128 devices in a mesh: space: 8 (over z_lo, x), mode: 16 (over z_hi, y, core).
Axes of the slice: x: 4, y: 4, z: 4 (z_hi: 2, z_lo: 2; z = z_hi * 2 + z_lo), core: 2. Of those that a mesh axis runs over, the one named last changes fastest.
Arguments:
- excess_phonon_enthalpy: bfloat16 [768, 64, 128, 128], P('mode', 'space'), may hold values from -0.21972656 to 0.21972656
- thermal_offset: float32 [128, 128, 64], P('space', 'mode'), may hold values from -6 to 6
- state_specific_warmth_scaled: float32 [768], P('mode'), may hold values from 0.5 to 2
- scattering_lifetimes: float32 [768], P('mode'), may hold values from 0.5 to 50
- state_polarization_label: int32 [768], P('mode'), may hold values from 0 to 5
- state_orientation_label: int32 [768], P('mode'), may hold values from 0 to 15
- polarization_propagation_rate: float32 [6], replicated, may hold values from 0.3 to 1
- thermal_conductance_bulk: float32 [128, 128, 64], P('space', 'mode'), may hold values from 0.25 to 1
- substance_label: int32 [128, 128, 64], P('space', 'mode'), may hold values 0 or 1
Outputs:
- final_temperature: float32 [128, 128, 64], P('space', 'mode')
- heat_flux: float32 [3, 128, 128, 64], P(None, 'space', 'mode')
The draws below stay inside these ranges and needn't reach their ends.
Inputs may be any that keep to these rules, and one draw needn't show every extreme that they name: `substance_label`: 1 marks a pore cell.
All inputs are finite; a program needn't handle non-finite values. No bound on the sum of `substance_label` on one device may be relied on, other than what follows from the above.
Results may differ from the reference program's by a relative error of at most 0.0028.
Values may be sent and summed in bfloat16 or wider, within the bound.
No kernel may reach another device: no remote copies, remote signals or barrier semaphores. Data moves between devices by JAX's collectives and lax.ppermute only.
A program may use at most 128 MiB of HBM per device.

```python
import math
import jax
import jax.numpy as jnp
from jax import lax

M = 768
NB = 6
ND = 16
SWEEPS = 4
OUTER = 2
LATTICE_EAST = 128
LATTICE_NORTH = 128
LATTICE_UPWARD = 64


def touch_ends(drawn, key, low, high):
    longest = drawn.shape.index(max(drawn.shape))
    spots = []
    for shift in (0, 1):
        where = [jax.random.randint(jax.random.fold_in(key, axis), (), 0, length) for axis, length in enumerate(drawn.shape)]
        where[longest] = (where[longest] + shift) % drawn.shape[longest]
        spots.append(tuple(where))
    return drawn.at[spots[0]].set(low).at[spots[1]].set(high)


def level_of(stream_key, extent, pieces, low, largest):
    def one(dim, shards_of):
        draws = jax.random.uniform(jax.random.fold_in(jax.random.fold_in(stream_key, 6), dim), (shards_of,), jnp.float32, low / len(pieces), largest / len(pieces))
        return jnp.repeat(jnp.exp(draws), extent[dim] // shards_of).reshape((-1,) + (1,) * (len(extent) - dim - 1))

    gain = one(*pieces[0])
    for cut in pieces[1:]:
        gain = gain * one(*cut)
    return gain


def scatter_about(stream_key, shape, scale, limit, cuts=(), kind=jnp.bfloat16):
    drawn = scale * jax.random.normal(stream_key, shape, jnp.float32)
    if cuts:
        drawn = drawn * level_of(stream_key, shape, cuts, -0.22, 0.18)
    return jnp.clip(drawn, -limit, limit).astype(kind)


def setup_inputs(seed: int = 0) -> dict:
    seeds = jax.random.split(jax.random.key(seed), 10)
    excess_phonon_enthalpy = scatter_about(seeds[0], (M, LATTICE_UPWARD, LATTICE_EAST, LATTICE_NORTH), 0.036, 0.21972656, ((0, 16), (1, 8)))
    thermal_offset = scatter_about(seeds[1], (LATTICE_EAST, LATTICE_NORTH, LATTICE_UPWARD), 1.0, 6.0, ((0, 8), (1, 16)), jnp.float32)
    state_specific_warmth_scaled = jnp.clip(jnp.exp(math.log(2.0) - 1.3862944 * jax.random.uniform(seeds[2], (M,), jnp.float32) ** level_of(seeds[2], (M,), ((0, 16),), -0.2, 0.2)), 0.5, 2.0)
    scattering_lifetimes = jnp.clip(jnp.exp(math.log(50.0) - 4.6051702 * jax.random.uniform(seeds[3], (M,), jnp.float32) ** level_of(seeds[3], (M,), ((0, 16),), -0.2, 0.2)), 0.5, 50.0)
    state_polarization_label = touch_ends(jax.random.randint(seeds[4], (M,), 0, NB), jax.random.fold_in(seeds[4], 1), 0, NB - 1).astype(jnp.int32)
    state_orientation_label = touch_ends(jax.random.randint(seeds[5], (M,), 0, ND), jax.random.fold_in(seeds[5], 1), 0, ND - 1).astype(jnp.int32)
    polarization_propagation_rate = jnp.clip(jnp.exp(jax.random.uniform(seeds[6], (NB,), jnp.float32, math.log(0.3), math.log(1.0))), 0.3, 1.0)
    thermal_conductance_bulk = jnp.clip(0.25 + 0.75 * jax.random.uniform(seeds[7], (LATTICE_EAST, LATTICE_NORTH, LATTICE_UPWARD), jnp.float32) ** level_of(seeds[7], (LATTICE_EAST, LATTICE_NORTH, LATTICE_UPWARD), ((0, 8), (1, 16)), -0.2, 0.2), 0.25, 1.0)
    substance_label = touch_ends((jax.random.randint(seeds[8], (LATTICE_EAST, LATTICE_NORTH, LATTICE_UPWARD), 0, 4) < 1).astype(jnp.int32), jax.random.fold_in(seeds[8], 1), 0, 1)
    return {"excess_phonon_enthalpy": excess_phonon_enthalpy, "thermal_offset": thermal_offset, "state_specific_warmth_scaled": state_specific_warmth_scaled, "scattering_lifetimes": scattering_lifetimes, "state_polarization_label": state_polarization_label, "state_orientation_label": state_orientation_label, "polarization_propagation_rate": polarization_propagation_rate, "thermal_conductance_bulk": thermal_conductance_bulk, "substance_label": substance_label}


time_step = 0.25
pore_factor = 0.1
kappa_top = 1.0

def mode_table(state_polarization_label, state_orientation_label, state_specific_warmth_scaled, scattering_lifetimes, polarization_propagation_rate):
    branches = jnp.arange(polarization_propagation_rate.shape[0], dtype=jnp.int32)
    onehot = (state_polarization_label[:, None] == branches[None, :]).astype(jnp.float32)
    speed = lax.optimization_barrier(jnp.sum(onehot * polarization_propagation_rate[None, :], axis=1))
    polar = state_orientation_label // 4
    azimuth = state_orientation_label % 4
    cosine = (2 * polar + 1).astype(jnp.float32) * 0.25 - 1.0
    sine = jnp.sqrt(1.0 - cosine * cosine)
    angle = (azimuth.astype(jnp.float32) + 0.5) * (math.pi / 2.0)
    velocity = (speed * sine * jnp.cos(angle), speed * sine * jnp.sin(angle), speed * cosine)
    rates = 1.0 / scattering_lifetimes
    capacity = state_specific_warmth_scaled / float(M)
    return (velocity, rates, capacity)

def upwind(padded, temp_slab, along_x, along_y, along_z, rates, capacity):

    def widen(values):
        return values[:, None, None, None]
    current = padded[:, 1:-1]
    z_before = padded[:, :-2]
    z_after = padded[:, 2:]
    x_padded = jnp.pad(current, ((0, 0), (0, 0), (1, 1), (0, 0)))
    y_padded = jnp.pad(current, ((0, 0), (0, 0), (0, 0), (1, 1)))

    def advect(speed, before, after):
        flow = widen(speed)
        return jnp.maximum(flow, 0.0) * (current - before) + jnp.minimum(flow, 0.0) * (after - current)
    total_advect = advect(along_x, x_padded[:, :, :-2], x_padded[:, :, 2:])
    total_advect = total_advect + advect(along_y, y_padded[:, :, :, :-2], y_padded[:, :, :, 2:])
    total_advect = total_advect + advect(along_z, z_before, z_after)
    updated = current - time_step * total_advect + time_step * widen(rates) * (widen(capacity) * temp_slab[None] - current)
    weights = jnp.stack([rates, along_x, along_y, along_z])
    moments = jnp.einsum('km,mzxy->kzxy', weights, updated, precision=lax.Precision.HIGHEST)
    return (updated, moments)

def harmonic(first, second):
    summed = first + second
    positive = summed > 0.0
    return jnp.where(positive, 2.0 * first * second / jnp.where(positive, summed, 1.0), 0.0)

def face_table(kappa_ext):
    center = kappa_ext[1:-1, 1:-1]
    z_padded = jnp.pad(center, ((0, 0), (0, 0), (1, 1)))
    return (harmonic(center, kappa_ext[2:, 1:-1]), harmonic(kappa_ext[:-2, 1:-1], center), harmonic(center, kappa_ext[1:-1, 2:]), harmonic(kappa_ext[1:-1, :-2], center), harmonic(center, z_padded[:, :, 2:]), harmonic(z_padded[:, :, :-2], center))

def crop(values, matrix_height, matrix_breadth):
    top = (values.shape[0] - matrix_height) // 2
    left = (values.shape[1] - matrix_breadth) // 2
    return values[top:top + matrix_height, left:left + matrix_breadth]

def apply_operator(padded, faces, total):
    matrix_height = padded.shape[0] - 2
    matrix_breadth = padded.shape[1] - 2
    cut = [crop(face, matrix_height, matrix_breadth) for face in faces]
    center = padded[1:-1, 1:-1]
    z_padded = jnp.pad(center, ((0, 0), (0, 0), (1, 1)))
    spread = cut[0] * (padded[2:, 1:-1] - center) + cut[1] * (padded[:-2, 1:-1] - center)
    spread = spread + cut[2] * (padded[1:-1, 2:] - center) + cut[3] * (padded[1:-1, :-2] - center)
    spread = spread + cut[4] * (z_padded[:, :, 2:] - center) + cut[5] * (z_padded[:, :, :-2] - center)
    return total * center - spread

def divergence(fluxes):
    z_flux = jnp.pad(fluxes[2][1:-1, 1:-1], ((0, 0), (0, 0), (1, 1)))
    summed = fluxes[0][2:, 1:-1] - fluxes[0][:-2, 1:-1] + (fluxes[1][1:-1, 2:] - fluxes[1][1:-1, :-2])
    summed = summed + (z_flux[:, :, 2:] - z_flux[:, :, :-2])
    return summed * 0.5

def chebyshev(rhs, faces, total, extend, matrix_height, matrix_breadth):
    theta = total + 6.0 * kappa_top
    spread = 6.0 * kappa_top
    sigma = theta / spread
    rho = 1.0 / sigma
    residual = rhs
    direction = rhs / theta
    correction = jnp.zeros((matrix_height, matrix_breadth, rhs.shape[2]), jnp.float32)
    for sweep in range(SWEEPS):
        correction = correction + crop(direction, matrix_height, matrix_breadth)
        if sweep < SWEEPS - 1:
            image = apply_operator(extend(direction), faces, total)
            residual = crop(residual, image.shape[0], image.shape[1]) - image
            rho_next = 1.0 / (2.0 * sigma - rho)
            direction = rho_next * rho * crop(direction, image.shape[0], image.shape[1]) + 2.0 * rho_next / spread * residual
            rho = rho_next
    return correction

def pad_cycle(values):
    return jnp.pad(values, ((1, 1), (1, 1), (0, 0)))

def reference(excess_phonon_enthalpy, thermal_offset, state_specific_warmth_scaled, scattering_lifetimes, state_polarization_label, state_orientation_label, polarization_propagation_rate, thermal_conductance_bulk, substance_label):
    velocity, rates, capacity = mode_table(state_polarization_label, state_orientation_label, state_specific_warmth_scaled, scattering_lifetimes, polarization_propagation_rate)
    total = jnp.sum(capacity * rates)
    kappa = thermal_conductance_bulk * jnp.where(substance_label == 1, pore_factor, 1.0)
    faces = face_table(pad_cycle(kappa))
    spatial_entries = thermal_offset
    state = excess_phonon_enthalpy
    group = 16
    fluxes = None
    for outer in range(OUTER):
        temp_slab = jnp.transpose(spatial_entries, (2, 0, 1))
        shaped = state.reshape(M // group, group, LATTICE_UPWARD, LATTICE_EAST, LATTICE_NORTH)
        params = (velocity[0].reshape(-1, group), velocity[1].reshape(-1, group), velocity[2].reshape(-1, group), rates.reshape(-1, group), capacity.reshape(-1, group))

        def step(carry, inputs):
            block, along_x, along_y, along_z, rate_part, cap_part = inputs
            padded = jnp.pad(block.astype(jnp.float32), ((0, 0), (1, 1), (0, 0), (0, 0)))
            updated, moments = upwind(padded, temp_slab, along_x, along_y, along_z, rate_part, cap_part)
            return (carry + moments, updated.astype(jnp.bfloat16))
        start = jnp.zeros((4, LATTICE_UPWARD, LATTICE_EAST, LATTICE_NORTH), jnp.float32)
        moments, news = lax.scan(step, start, (shaped,) + params)
        state = news.reshape(M, LATTICE_UPWARD, LATTICE_EAST, LATTICE_NORTH)
        blocks = jnp.transpose(moments, (0, 2, 3, 1))
        fluxes = blocks[1:]
        rhs = -divergence(jnp.pad(fluxes, ((0, 0), (1, 1), (1, 1), (0, 0))))
        correction = chebyshev(rhs, faces, total, pad_cycle, LATTICE_EAST, LATTICE_NORTH)
        spatial_entries = blocks[0] / total + correction
    return (spatial_entries, fluxes)
```

```python
import math

import jax
import jax.numpy as jnp
from jax import lax
from jax.experimental import pallas as pl
from jax.experimental.pallas import tpu as pltpu
from jax.sharding import Mesh, PartitionSpec as P


SWEEPS = 4
STEP = 0.25
MODES = 768
LOCAL = 48
SLAB = 8
NX = 128
NY = 128
WIN = 5 * LOCAL
DEPTH = 256
EXT = 12
PITCH = 17
ROWS = 6 * EXT * 8
PIECE = ROWS + 16
F32 = jnp.float32
BF16 = jnp.bfloat16

SHIFTS = (
    (0, 0), (1, 0), (-1, 0), (2, 0), (-2, 0),
    (0, 1), (1, 1), (-1, 1),
    (0, -1), (1, -1), (-1, -1),
    (0, 2), (0, -2),
)
NS = len(SHIFTS)
BY_Z = tuple(
    (sz, tuple((sy, n) for n, (sy, z) in enumerate(SHIFTS) if z == sz)) for sz in (-2, -1, 0, 1, 2)
)


def lane_iota(shape):
    return lax.broadcasted_iota(jnp.int32, shape, len(shape) - 1)


def mode_rows(table, prop_ref):
    branch = table[0:1]
    orient = table[1:2]
    cap = table[2:3] / float(MODES)
    rate = 1.0 / table[3:4]
    speed = jnp.zeros_like(branch)
    for b in range(6):
        speed = speed + jnp.where(branch == float(b), prop_ref[b], 0.0)
    polar = jnp.where(orient >= 4.0, 1.0, 0.0) + jnp.where(orient >= 8.0, 1.0, 0.0)
    polar = polar + jnp.where(orient >= 12.0, 1.0, 0.0)
    turn = orient - 4.0 * polar
    cosine = (2.0 * polar + 1.0) * 0.25 - 1.0
    sine = jnp.sqrt(1.0 - cosine * cosine)
    half = math.sqrt(0.5)
    east = jnp.where((turn == 0.0) | (turn == 3.0), half, -half)
    north = jnp.where(turn < 2.0, half, -half)
    return speed * sine * east, speed * sine * north, speed * cosine, rate, cap


def step_terms(vx, vy, vz, rate):
    cx, cy, cz = (STEP * jnp.abs(v) for v in (vx, vy, vz))
    c0 = 1.0 - cx - cy - cz - STEP * rate
    one = (((0, 0, 0), c0), ((1, 0, 0), cx), ((0, 1, 0), cy), ((0, 0, 1), cz))
    two = (
        ((0, 0, 0), c0 * c0),
        ((1, 0, 0), 2.0 * c0 * cx),
        ((0, 1, 0), 2.0 * c0 * cy),
        ((0, 0, 1), 2.0 * c0 * cz),
        ((2, 0, 0), cx * cx),
        ((0, 2, 0), cy * cy),
        ((0, 0, 2), cz * cz),
        ((1, 1, 0), 2.0 * cx * cy),
        ((1, 0, 1), 2.0 * cx * cz),
        ((0, 1, 1), 2.0 * cy * cz),
    )
    return one, two


def fields_on_rows(vx, vy, vz, rate):
    lanes = rate.shape[1]
    row = lax.broadcasted_iota(jnp.int32, (8, lanes), 0) % 4
    full = [jnp.broadcast_to(v, (8, lanes)) for v in (rate, vx, vy, vz)]
    return jnp.where(
        row == 0, full[0], jnp.where(row == 1, full[1], jnp.where(row == 2, full[2], full[3]))
    )


def build_tables(par_ref, prop_ref, par5, coef):
    par5[...] = jnp.ones(par5.shape, F32)
    for o in range(5):
        par5[0:4, o * LOCAL : (o + 1) * LOCAL] = par_ref[...]
    vx, vy, vz, rate, _ = mode_rows(par5[0:4, :], prop_ref)
    one, two = step_terms(vx, vy, vz, rate)
    weights = fields_on_rows(vx, vy, vz, rate)
    lane = lane_iota((1, DEPTH))
    offset = -2.0 + sum(jnp.where(lane >= o * LOCAL, 1.0, 0.0) for o in range(1, 5))
    inside = lane < WIN
    dx, dy, dz = (jnp.where(v > 0.0, 1.0, -1.0) for v in (vx, vy, vz))
    upper = lax.broadcasted_iota(jnp.int32, (8, DEPTH), 0) < 4

    def total(terms, sy, sz):
        out = jnp.zeros((1, DEPTH), F32)
        for (ax, ay, az), value in terms:
            if ay != abs(sy) or az != abs(sz):
                continue
            hit = inside & (offset == -float(ax) * dx)
            if ay:
                hit = hit & (dy * float(ay) == float(sy))
            if az:
                hit = hit & (dz * float(az) == float(sz))
            out = out + jnp.where(hit, value, 0.0)
        return jnp.broadcast_to(out, (8, DEPTH))

    parts = [
        weights * jnp.where(upper, total(one, sy, sz), total(two, sy, sz)) for sy, sz in SHIFTS
    ]
    rest = parts[0] - parts[0].astype(BF16).astype(F32)
    coef[...] = jnp.concatenate(parts + [rest], axis=0).astype(BF16)


def mode_sums(par_ref, prop_ref, core):
    vx, vy, vz, rate, cap = mode_rows(par_ref[...], prop_ref)
    one, _ = step_terms(vx, vy, vz, rate)
    weights = fields_on_rows(vx, vy, vz, rate)
    gain = STEP * rate * cap
    columns = [weights * gain * one[0][1]]
    for ((ax, ay, az), value), v in zip(one[1:], (vx, vy, vz)):
        for sign in (1.0, -1.0):
            columns.append(weights * gain * jnp.where(v * sign > 0.0, value, 0.0))
    columns.append(weights * gain)
    columns.append(jnp.broadcast_to(cap * rate, weights.shape))
    lane = lane_iota((8, 128))
    sums = jnp.zeros((8, 128), F32)
    for n, column in enumerate(columns):
        sums = jnp.where(lane == n, jnp.sum(column, axis=1, keepdims=True), sums)
    high = sums.astype(BF16).astype(F32)
    rest = sums - high
    middle = rest.astype(BF16).astype(F32)
    low = rest - middle
    packed = high + pltpu.roll(middle, 16, 1) + pltpu.roll(low, 32, 1)
    packed = jnp.where(core == 0, packed, pltpu.roll(packed, 64, 1))
    return jnp.concatenate([packed, jnp.zeros((8, 128), F32)], axis=0).astype(BF16)


def moments_kernel(idx_ref, prop_ref, par_ref, e_ref, keep_ref, send_ref, par5, coef, spread, turned, acc):
    z = pl.program_id(0)
    space = idx_ref[0]
    core = idx_ref[1]
    LAYER = NX * 8

    @pl.when(z == 0)
    def _():
        build_tables(par_ref, prop_ref, par5, coef)
        turned[0 : 2 * LOCAL, :] = jnp.zeros((2 * LOCAL, 128), BF16)
        turned[(NX + 2) * LOCAL :, :] = jnp.zeros((2 * LOCAL + 16, 128), BF16)

        @pl.loop(0, 5 * LAYER // 64)
        def _(r):
            acc[pl.ds(pl.multiple_of(r * 64, 64), 64), :] = jnp.zeros((64, 128), F32)

        acc[13 * LAYER : 14 * LAYER, :] = jnp.zeros((LAYER, 128), F32)

    @pl.loop(0, NX // 16)
    def _(c):
        x0 = pl.multiple_of(c * 16, 16)
        for m in range(LOCAL):
            spread[m * PITCH : m * PITCH + 16, :] = e_ref[m, 0, pl.ds(x0, 16), :].astype(F32)
        for xx in range(16):
            rows = spread[pl.ds(xx, LOCAL, stride=PITCH), :].astype(BF16)
            turned[pl.ds(pl.multiple_of((x0 + (xx + 2)) * LOCAL, 16), LOCAL), :] = rows

    lane = lane_iota((8, 128))

    def moved(value, sy):
        if sy == 0:
            return value
        rolled = pltpu.roll(value, sy % 128, 1)
        return jnp.where(lane >= sy if sy > 0 else lane < 128 + sy, rolled, 0.0)

    def one_pair(x):
            first = turned[x * LOCAL : x * LOCAL + DEPTH, :]
            second = turned[(x + 1) * LOCAL : (x + 1) * LOCAL + DEPTH, :]
            block = jnp.concatenate([first, second], axis=1)
            out = jnp.dot(coef[...], block, preferred_element_type=F32)
            for half in range(2):
                for sz, members in BY_Z:
                    total = None
                    for sy, n in members:
                        part = moved(out[8 * n : 8 * n + 8, 128 * half : 128 * half + 128], sy)
                        if n == 0:
                            part = part + out[8 * NS :, 128 * half : 128 * half + 128]
                        total = part if total is None else total + part
                    at = pl.multiple_of((z + 3 + sz) * LAYER + (x + half) * 8, 8)
                    if sz == 2:
                        acc[pl.ds(at, 8), :] = total
                    else:
                        acc[pl.ds(at, 8), :] += total

    for x in range(0, NX, 2):
        one_pair(x)

    @pl.when(z == SLAB - 1)
    def _():
        @pl.when(space == 0)
        def _():
            acc[LAYER : 3 * LAYER, :] = jnp.zeros((2 * LAYER, 128), F32)

        @pl.when(space == 7)
        def _():
            acc[11 * LAYER : 13 * LAYER, :] = jnp.zeros((2 * LAYER, 128), F32)

        def give(ref, block, at, tile):
            ref[block, pl.ds(at, 16), :] = tile.astype(ref.dtype)

        row = lax.broadcasted_iota(jnp.int32, (NX, 128), 0)
        col = lane_iota((NX, 128))

        def layer(zo, field, shift=0):
            return acc[pl.ds((zo + 1) * LAYER + field + 8 * shift, NX, stride=8), :]

        def divergence(zo):
            east = jnp.where(row < NX - 1, layer(zo, 1, 1), 0.0)
            west = jnp.where(row > 0, layer(zo, 1, -1), 0.0)
            along_y = layer(zo, 2)
            north = jnp.where(col < 127, pltpu.roll(along_y, 127, 1), 0.0)
            south = jnp.where(col > 0, pltpu.roll(along_y, 1, 1), 0.0)
            up = layer(zo + 1, 3)
            down = layer(zo - 1, 3)
            return 0.5 * ((east - west) + (north - south) + (up - down))

        sources = (
            lambda zo: layer(zo, 0),
            divergence,
            lambda zo: layer(zo, 5),
            lambda zo: layer(zo, 6),
            lambda zo: layer(zo, 7),
            lambda zo: layer(zo, 4),
        )
        for f, source in enumerate(sources):

            @pl.loop(0, EXT // 2)
            def _(pair):
                zo = pair * 2
                even = source(zo).T
                odd = source(zo + 1).T
                at = pl.multiple_of((f * EXT + zo) * 8, 16)
                tiles = [
                    jnp.concatenate([even[8 * j : 8 * j + 8], odd[8 * j : 8 * j + 8]], axis=0)
                    for j in range(16)
                ]

                @pl.when(core == 0)
                def _():
                    for j in range(16):
                        give(send_ref if j % 2 else keep_ref, j // 2, at, tiles[j])

                @pl.when(core == 1)
                def _():
                    for j in range(16):
                        give(keep_ref if j % 2 else send_ref, j // 2, at, tiles[j])

        sums = mode_sums(par_ref, prop_ref, core)
        for p in range(8):
            keep_ref[p, ROWS:PIECE, :] = sums.astype(F32)
            send_ref[p, ROWS:PIECE, :] = sums


def moments(idx, prop, par, state):
    whole = pl.BlockSpec((8, PIECE, 128), lambda z: (0, 0, 0))
    return pl.pallas_call(
        moments_kernel,
        grid=(SLAB,),
        in_specs=[
            pl.BlockSpec(memory_space=pltpu.SMEM),
            pl.BlockSpec(memory_space=pltpu.SMEM),
            pl.BlockSpec((4, LOCAL), lambda z: (0, 0)),
            pl.BlockSpec((LOCAL, 1, NX, NY), lambda z: (0, z, 0, 0)),
        ],
        out_specs=[whole, whole],
        out_shape=[jax.ShapeDtypeStruct((8, PIECE, 128), t) for t in (F32, BF16)],
        scratch_shapes=[
            pltpu.VMEM((8, DEPTH), F32),
            pltpu.VMEM((NS * 8 + 8, DEPTH), BF16),
            pltpu.VMEM((LOCAL * PITCH + 8, 128), F32),
            pltpu.VMEM(((NX + 4) * LOCAL + 16, 128), BF16),
            pltpu.VMEM((14 * NX * 8, 128), F32),
        ],
        compiler_params=pltpu.CompilerParams(vmem_limit_bytes=48 << 20),
        cost_estimate=pl.CostEstimate(flops=20_000_000_000, bytes_accessed=16_000_000, transcendentals=0),
        name="moments",
    )(idx, prop, par, state)


def owner_kernel(got_ref, out_ref, sums_ref):
    lane = lane_iota((8, 128))
    part = lane % 32
    for f in range(6):
        for high in range(EXT // 4):
            base = (f * EXT + high * 4) * 8
            layers = got_ref[0, base : base + 32, :].astype(F32)
            for m in range(1, 8):
                layers = layers + got_ref[m, base : base + 32, :].astype(F32)
            tiles = []
            for i in range(8):
                value = None
                for low in range(4):
                    rolled = pltpu.roll(layers[8 * low : 8 * low + 8], (32 * low - 16 * i + 8) % 128, 1)
                    value = rolled if low == 0 else jnp.where(lane >= 32 * low, rolled, value)
                if i == 0:
                    value = jnp.where(part >= 8, value, 0.0)
                if i == 7:
                    value = jnp.where(part < 24, value, 0.0)
                tiles.append(value)
            at = (f * 3 + high) * 8
            for i in range(8):
                out_ref[i, at : at + 8, :] = tiles[i].astype(BF16)
                if f in (2, 3, 4):
                    low = tiles[i] - tiles[i].astype(BF16).astype(F32)
                    out_ref[i, at + 96 : at + 104, :] = low.astype(BF16)
    total = got_ref[0, ROWS:PIECE, :].astype(F32)
    for m in range(1, 8):
        total = total + got_ref[m, ROWS:PIECE, :].astype(F32)
    total = total[0:8]
    total = total + pltpu.roll(total, 64, 1)
    sums_ref[...] = total + pltpu.roll(total, 112, 1) + pltpu.roll(total, 96, 1)


def at_owner(got):
    return pl.pallas_call(
        owner_kernel,
        out_shape=[
            jax.ShapeDtypeStruct((8, 216, 128), BF16),
            jax.ShapeDtypeStruct((8, 128), F32),
        ],
        name="owner",
    )(got)


def merge_kernel(got_ref, known_ref, own_ref, halo_ref):
    group = lane_iota((8, 128)) // 32

    def layer(s, f, zo, quarter):
        at = (f * 3 + zo // 4) * 8
        value = got_ref[s, at : at + 8, :].astype(F32)
        if f in (2, 3, 4):
            value = value + got_ref[s, at + 96 : at + 104, :].astype(F32)
        turn = (32 * (quarter - zo % 4)) % 128
        return pltpu.roll(value, turn, 1) if turn else value

    for f in range(6):
        for zz in range(16):
            value = None
            for quarter in range(4):
                z = quarter * 16 + zz
                s = z // 8
                part = layer(s, f, z % 8 + 2, quarter)
                if z % 8 < 2 and s > 0:
                    part = part + layer(s - 1, f, z % 8 + 10, quarter)
                if z % 8 > 5 and s < 7:
                    part = part + layer(s + 1, f, z % 8 - 6, quarter)
                value = part if quarter == 0 else jnp.where(group >= quarter, part, value)
            own_ref[f, zz] = value
            if f < 5:
                halo_ref[(f * 16 + zz) * 8 : (f * 16 + zz) * 8 + 8, :] = value.astype(BF16)
    for n in range(2):
        halo_ref[640 + 128 * n : 768 + 128 * n, :] = known_ref[n].reshape(128, 128).astype(BF16)


def merged(got, known):
    return pl.pallas_call(
        merge_kernel,
        out_shape=[
            jax.ShapeDtypeStruct((6, 16, 8, 128), F32),
            jax.ShapeDtypeStruct((7 * 16 * 8, 128), BF16),
        ],
        name="merge",
    )(got, known)


def solve_kernel(idx_ref, sums_ref, own_ref, south_ref, north_ref, known_ref, temp_ref, flux_ref):
    lane = lane_iota((1, 24, 128))
    x = lane % 32 + (idx_ref[0] * 16 - 8)
    y = lax.broadcasted_iota(jnp.int32, (1, 24, 128), 1) + (idx_ref[1] * 8 - 8)
    inside = jnp.where((x >= 0) & (x < NX) & (y >= 0) & (y < NY), 1.0, 0.0)
    group = lane_iota((1, 24, 128)) // 32

    def wide(own, f):
        rows = slice(f * 128, f * 128 + 128)
        south = south_ref[rows, :].astype(F32).reshape(16, 8, 128)
        north = north_ref[rows, :].astype(F32).reshape(16, 8, 128)
        return jnp.concatenate([south, own, north], axis=1)

    def field(f):
        return wide(own_ref[f], f)

    def known(n):
        return wide(known_ref[n], 5 + n)

    def east(v):
        return pltpu.roll(v, 127, 2)

    def west(v):
        return pltpu.roll(v, 1, 2)

    def north(v):
        return jnp.concatenate([v[:, 1:], jnp.zeros((16, 1, 128), F32)], axis=1)

    def south(v):
        return jnp.concatenate([jnp.zeros((16, 1, 128), F32), v[:, :-1]], axis=1)

    def above(v):
        edge = jnp.where(group < 3, pltpu.roll(v[0:1], 96, 2), 0.0)
        return jnp.concatenate([v[1:], edge], axis=0)

    def below(v):
        edge = jnp.where(group > 0, pltpu.roll(v[15:16], 32, 2), 0.0)
        return jnp.concatenate([edge, v[:-1]], axis=0)

    total_scalar = sums_ref[0, 8]
    total = jnp.full((1, 24, 128), total_scalar, F32)
    theta = total + 6.0
    sigma = theta / 6.0
    kappa = known(1)

    def face(a, b):
        summed = a + b
        positive = summed > 0.0
        return jnp.where(positive, 2.0 * a * b / jnp.where(positive, summed, 1.0), 0.0)

    face_e = face(kappa, east(kappa))
    face_n = face(kappa, north(kappa))
    face_u = face(kappa, above(kappa))
    face_w = west(face_e)
    face_s = south(face_n)
    face_d = below(face_u)

    def operator(v):
        out = face_e * (east(v) - v) + face_w * (west(v) - v)
        out = out + face_n * (north(v) - v) + face_s * (south(v) - v)
        out = out + face_u * (above(v) - v) + face_d * (below(v) - v)
        return total * v - out

    def chebyshev(rhs):
        rho = 1.0 / sigma
        residual = rhs
        direction = rhs / theta
        correction = direction
        for _ in range(SWEEPS - 1):
            residual = residual - operator(direction)
            rho_next = 1.0 / (2.0 * sigma - rho)
            direction = rho_next * rho * direction + 2.0 * rho_next / 6.0 * residual
            rho = rho_next
            correction = correction + direction
        return correction

    temp = known(0)
    moved = (temp, west(temp), east(temp), south(temp), north(temp), below(temp), above(temp))
    gain = [sums_ref[k, 7] for k in range(4)]
    rhs = 0.5 * (
        gain[1] * (moved[2] - moved[1]) + gain[2] * (moved[4] - moved[3]) + gain[3] * (moved[6] - moved[5])
    )
    rhs = -(field(1) + rhs)
    once = (field(0) + gain[0] * temp) / total + chebyshev(rhs)

    def second(k, part):
        value = part + gain[k] * once
        for s in range(7):
            value = value + sums_ref[k, s] * moved[s]
        return value

    flux = [second(k, field(k + 1)) * inside for k in (1, 2, 3)]
    own = own_ref[5]
    energy = second(0, jnp.concatenate([own, own, own], axis=1))
    rhs = -0.5 * (
        (east(flux[0]) - west(flux[0])) + (north(flux[1]) - south(flux[1])) + (above(flux[2]) - below(flux[2]))
    )
    twice = energy / total + chebyshev(rhs)
    temp_ref[...] = twice[:, 8:16]
    for n in range(3):
        flux_ref[n] = flux[n][:, 8:16]


def solved(idx, sums, own, south, north, known):
    vmem = pl.BlockSpec(memory_space=pltpu.VMEM)
    smem = pl.BlockSpec(memory_space=pltpu.SMEM)
    return pl.pallas_call(
        solve_kernel,
        in_specs=[smem, smem] + [vmem] * 4,
        out_specs=[vmem, vmem],
        out_shape=[
            jax.ShapeDtypeStruct((16, 8, 128), F32),
            jax.ShapeDtypeStruct((3, 16, 8, 128), F32),
        ],
        compiler_params=pltpu.CompilerParams(vmem_limit_bytes=48 << 20),
        name="solve",
    )(idx, sums, own, south, north, known)


LINE = ("zy", "core")


def both_ways(value, axis, count):
    ahead = [(i, i + 1) for i in range(count - 1)]
    behind = [(i + 1, i) for i in range(count - 1)]
    if isinstance(value, tuple):
        tail, head = value
    else:
        tail = head = value
    return lax.ppermute(tail, axis, ahead), lax.ppermute(head, axis, behind)


def per_device(
    excess_phonon_enthalpy,
    thermal_offset,
    state_specific_warmth_scaled,
    scattering_lifetimes,
    state_polarization_label,
    state_orientation_label,
    polarization_propagation_rate,
    thermal_conductance_bulk,
    substance_label,
):
    space = lax.axis_index("space")
    core = lax.axis_index("core")
    line = lax.axis_index("zy") * 2 + core
    kappa = thermal_conductance_bulk * jnp.where(substance_label == 1, 0.1, 1.0)
    known = jnp.stack([thermal_offset, kappa])
    west, east = both_ways((known[:, 8:], known[:, :8]), "space", 8)
    known = jnp.concatenate([west, known, east], axis=1)
    known = known.reshape(2, 32, 8, 4, 16).transpose(0, 4, 2, 3, 1).reshape(2, 16, 8, 128)

    table = jnp.stack(
        [
            state_polarization_label.astype(F32),
            state_orientation_label.astype(F32),
            state_specific_warmth_scaled,
            scattering_lifetimes,
        ]
    )
    keep, send = moments(
        jnp.stack([space, core]).astype(jnp.int32),
        polarization_propagation_rate,
        table,
        excess_phonon_enthalpy,
    )
    received = lax.ppermute(send, "core", [(0, 1), (1, 0)])
    paired = (keep.astype(F32) + received.astype(F32)).astype(BF16)
    got = lax.all_to_all(paired, "zy", 0, 0, tiled=True)
    pieces, sums = at_owner(got)
    pieces = lax.all_to_all(pieces, "space", 0, 0, tiled=True)
    own, halo = merged(pieces, known)
    south, north = both_ways(halo, LINE, 16)
    temp, flux = solved(jnp.stack([space, line]).astype(jnp.int32), sums, own, south, north, known)

    def unpacked(value):
        lead = value.shape[:-3]
        n = len(lead)
        value = value.reshape(lead + (16, 8, 4, 32))[..., 8:24]
        order = tuple(range(n)) + tuple(n + d for d in (3, 1, 2, 0))
        return value.transpose(order).reshape(lead + (16, 8, 64))

    return unpacked(temp), unpacked(flux)


def solution(mesh):
    parts = Mesh(mesh.devices.reshape(8, 8, 2), ("space", "zy", "core"))
    modes = P(LINE)
    block = P("space", LINE, None)
    return jax.shard_map(
        per_device,
        mesh=parts,
        in_specs=(P(LINE, "space", None, None), block, modes, modes, modes, modes, P(), block, block),
        out_specs=(block, P(None, "space", LINE, None)),
        check_vma=False,
    )
```

```python
import math

import jax
import jax.numpy as jnp
from jax import lax
from jax.experimental import pallas as pl
from jax.experimental.pallas import tpu as pltpu
from jax.sharding import Mesh, PartitionSpec as P

SWEEPS = 4
STEP = 0.25
MODES = 768
LOCAL = 48
SLAB = 8
NX = 128
NY = 128
NZ = 64
WIN = 5 * LOCAL
DEPTH = 256
EXT = 12
PITCH = 17
PACE = 9
LAYERS = 6 * EXT
DEPTHS = LAYERS // 8
PIECE = DEPTHS * 8
F32 = jnp.float32
BF16 = jnp.bfloat16

SHIFTS = (
    (0, 0), (1, 0), (-1, 0), (2, 0), (-2, 0),
    (0, 1), (1, 1), (-1, 1),
    (0, -1), (1, -1), (-1, -1),
    (0, 2), (0, -2),
)
NS = len(SHIFTS)
BY_Z = tuple(
    (sz, tuple((sy, n) for n, (sy, z) in enumerate(SHIFTS) if z == sz)) for sz in (-2, -1, 0, 1, 2)
)


def lane_iota(shape):
    return lax.broadcasted_iota(jnp.int32, shape, len(shape) - 1)


def mode_rows(table, prop_ref):
    branch = table[0:1]
    orient = table[1:2]
    cap = table[2:3] / float(MODES)
    rate = 1.0 / table[3:4]
    speed = jnp.zeros_like(branch)
    for b in range(6):
        speed = speed + jnp.where(branch == float(b), prop_ref[b], 0.0)
    polar = jnp.where(orient >= 4.0, 1.0, 0.0) + jnp.where(orient >= 8.0, 1.0, 0.0)
    polar = polar + jnp.where(orient >= 12.0, 1.0, 0.0)
    turn = orient - 4.0 * polar
    cosine = (2.0 * polar + 1.0) * 0.25 - 1.0
    sine = jnp.sqrt(1.0 - cosine * cosine)
    half = math.sqrt(0.5)
    east = jnp.where((turn == 0.0) | (turn == 3.0), half, -half)
    north = jnp.where(turn < 2.0, half, -half)
    return speed * sine * east, speed * sine * north, speed * cosine, rate, cap


def step_terms(vx, vy, vz, rate):
    cx, cy, cz = (STEP * jnp.abs(v) for v in (vx, vy, vz))
    c0 = 1.0 - cx - cy - cz - STEP * rate
    one = (((0, 0, 0), c0), ((1, 0, 0), cx), ((0, 1, 0), cy), ((0, 0, 1), cz))
    two = (
        ((0, 0, 0), c0 * c0),
        ((1, 0, 0), 2.0 * c0 * cx),
        ((0, 1, 0), 2.0 * c0 * cy),
        ((0, 0, 1), 2.0 * c0 * cz),
        ((2, 0, 0), cx * cx),
        ((0, 2, 0), cy * cy),
        ((0, 0, 2), cz * cz),
        ((1, 1, 0), 2.0 * cx * cy),
        ((1, 0, 1), 2.0 * cx * cz),
        ((0, 1, 1), 2.0 * cy * cz),
    )
    return one, two


def fields_on_rows(vx, vy, vz, rate):
    lanes = rate.shape[1]
    row = lax.broadcasted_iota(jnp.int32, (8, lanes), 0) % 4
    full = [jnp.broadcast_to(v, (8, lanes)) for v in (rate, vx, vy, vz)]
    return jnp.where(
        row == 0, full[0], jnp.where(row == 1, full[1], jnp.where(row == 2, full[2], full[3]))
    )


def build_tables(par_ref, prop_ref, par5, coef):
    par5[...] = jnp.ones(par5.shape, F32)
    for o in range(5):
        par5[0:4, o * LOCAL : (o + 1) * LOCAL] = par_ref[...]
    vx, vy, vz, rate, _ = mode_rows(par5[0:4, :], prop_ref)
    one, two = step_terms(vx, vy, vz, rate)
    weights = fields_on_rows(vx, vy, vz, rate)
    lane = lane_iota((1, DEPTH))
    offset = -2.0 + sum(jnp.where(lane >= o * LOCAL, 1.0, 0.0) for o in range(1, 5))
    inside = lane < WIN
    dx, dy, dz = (jnp.where(v > 0.0, 1.0, -1.0) for v in (vx, vy, vz))
    upper = lax.broadcasted_iota(jnp.int32, (8, DEPTH), 0) < 4

    def total(terms, sy, sz):
        out = jnp.zeros((1, DEPTH), F32)
        for (ax, ay, az), value in terms:
            if ay != abs(sy) or az != abs(sz):
                continue
            hit = inside & (offset == -float(ax) * dx)
            if ay:
                hit = hit & (dy * float(ay) == float(sy))
            if az:
                hit = hit & (dz * float(az) == float(sz))
            out = out + jnp.where(hit, value, 0.0)
        return jnp.broadcast_to(out, (8, DEPTH))

    parts = [
        weights * jnp.where(upper, total(one, sy, sz), total(two, sy, sz)) for sy, sz in SHIFTS
    ]
    rest = parts[0] - parts[0].astype(BF16).astype(F32)
    coef[...] = jnp.concatenate(parts + [rest], axis=0).astype(BF16)


def mode_sums(par_ref, prop_ref, core):
    vx, vy, vz, rate, cap = mode_rows(par_ref[...], prop_ref)
    one, _ = step_terms(vx, vy, vz, rate)
    weights = fields_on_rows(vx, vy, vz, rate)
    gain = STEP * rate * cap
    columns = [weights * gain * one[0][1]]
    for ((ax, ay, az), value), v in zip(one[1:], (vx, vy, vz)):
        for sign in (1.0, -1.0):
            columns.append(weights * gain * jnp.where(v * sign > 0.0, value, 0.0))
    columns.append(weights * gain)
    columns.append(jnp.broadcast_to(cap * rate, weights.shape))
    lane = lane_iota((8, 128))
    sums = jnp.zeros((8, 128), F32)
    for n, column in enumerate(columns):
        sums = jnp.where(lane == n, jnp.sum(column, axis=1, keepdims=True), sums)
    row = lax.broadcasted_iota(jnp.int32, (8, 128), 0)
    sums = jnp.where((row // 4) == core, sums, 0.0)
    high = sums.astype(BF16).astype(F32)
    return high, pltpu.roll(sums - high, 48, 1)


def moments_kernel(idx_ref, prop_ref, par_ref, e_ref, keep_ref, send_ref, par5, coef, spread, turned, acc, drift):
    z = pl.program_id(0)
    space = idx_ref[0]
    core = idx_ref[1]
    LAYER = NX * PACE

    @pl.when(z == 0)
    def _():
        build_tables(par_ref, prop_ref, par5, coef)
        turned[0 : 2 * LOCAL, :] = jnp.zeros((2 * LOCAL, 128), BF16)
        turned[(NX + 2) * LOCAL :, :] = jnp.zeros((2 * LOCAL + 16, 128), BF16)

        @pl.loop(0, 5 * LAYER // 64)
        def _(r):
            acc[pl.ds(pl.multiple_of(r * 64, 64), 64), :] = jnp.zeros((64, 128), F32)

        acc[13 * LAYER : 14 * LAYER, :] = jnp.zeros((LAYER, 128), F32)

    def turn(c):
        for m in range(LOCAL):
            at = (c * LOCAL + m) * PITCH
            spread[at : at + 16, :] = e_ref[m, 0, 16 * c : 16 * c + 16, :].astype(F32)
        for xx in range(16):
            rows = spread[pl.ds(c * LOCAL * PITCH + xx, LOCAL, stride=PITCH), :].astype(BF16)
            at = (16 * c + xx + 2) * LOCAL
            turned[at : at + LOCAL, :] = rows

    lane = lane_iota((8, 128))

    def moved(value, sy):
        if sy == 0:
            return value
        rolled = pltpu.roll(value, sy % 128, 1)
        return jnp.where(lane >= sy if sy > 0 else lane < 128 + sy, rolled, 0.0)

    def one_pair(x):
            first = turned[x * LOCAL : x * LOCAL + DEPTH, :]
            second = turned[(x + 1) * LOCAL : (x + 1) * LOCAL + DEPTH, :]
            block = jnp.concatenate([first, second], axis=1)
            out = jnp.dot(coef[...], block, preferred_element_type=F32)
            for half in range(2):
                for sz, members in BY_Z:
                    total = None
                    for sy, n in members:
                        part = moved(out[8 * n : 8 * n + 8, 128 * half : 128 * half + 128], sy)
                        if n == 0:
                            part = part + out[8 * NS :, 128 * half : 128 * half + 128]
                        total = part if total is None else total + part
                    at = (z + 3 + sz) * LAYER + (x + half) * PACE
                    if sz == 2:
                        acc[pl.ds(at, 8), :] = total
                    else:
                        acc[pl.ds(at, 8), :] += total

    CHUNKS = NX // 16
    turn(0)
    for c in range(CHUNKS):
        if c + 1 < CHUNKS:
            turn(c + 1)
        for x in range(16 * c, 16 * c + 16, 2):
            one_pair(x)

    @pl.when(z == SLAB - 1)
    def _():
        @pl.when(space == 0)
        def _():
            acc[LAYER : 3 * LAYER, :] = jnp.zeros((2 * LAYER, 128), F32)

        @pl.when(space == 7)
        def _():
            acc[11 * LAYER : 13 * LAYER, :] = jnp.zeros((2 * LAYER, 128), F32)

        row = lax.broadcasted_iota(jnp.int32, (NX, 128), 0)
        col = lane_iota((NX, 128))

        def layer(zo, field, shift=0):
            return acc[pl.ds((zo + 1) * LAYER + field + PACE * shift, NX, stride=PACE), :]

        def divergence(zo):
            east = jnp.where(row < NX - 1, layer(zo, 1, 1), 0.0)
            west = jnp.where(row > 0, layer(zo, 1, -1), 0.0)
            along_y = layer(zo, 2)
            north = jnp.where(col < 127, pltpu.roll(along_y, 127, 1), 0.0)
            south = jnp.where(col > 0, pltpu.roll(along_y, 1, 1), 0.0)
            up = layer(zo + 1, 3)
            down = layer(zo - 1, 3)
            return 0.5 * ((east - west) + (north - south) + (up - down))

        for zo in range(EXT):
            drift[zo * NX : zo * NX + NX, :] = divergence(zo)
        rows = (0, None, 5, 6, 7, 4)
        extras = mode_sums(par_ref, prop_ref, core)

        def strip(depth, i):
            f, zo = divmod(depth, EXT)
            if rows[f] is None:
                return drift[zo * NX + 16 * i : zo * NX + 16 * i + 16, :]
            return acc[pl.ds((zo + 1) * LAYER + rows[f] + 16 * i * PACE, 16, stride=PACE), :]

        for d in range(DEPTHS):
            for i in range(8):
                tile = jnp.concatenate([strip(8 * d + low, i) for low in range(8)], axis=0).T
                for p in range(8):
                    first, second = tile[16 * p : 16 * p + 8], tile[16 * p + 8 : 16 * p + 16]
                    kept = jnp.where(core == 0, first, second)
                    sent = jnp.where(core == 0, second, first)
                    if d < 2:
                        kept = kept + extras[d]
                        sent = sent + extras[d]
                    keep_ref[8 * i + p, 8 * d : 8 * d + 8, :] = kept
                    send_ref[8 * i + p, 8 * d : 8 * d + 8, :] = sent.astype(BF16)


def moments(idx, prop, par, state):
    whole = pl.BlockSpec((64, PIECE, 128), lambda z: (0, 0, 0))
    return pl.pallas_call(
        moments_kernel,
        grid=(SLAB,),
        in_specs=[
            pl.BlockSpec(memory_space=pltpu.SMEM),
            pl.BlockSpec(memory_space=pltpu.SMEM),
            pl.BlockSpec((4, LOCAL), lambda z: (0, 0)),
            pl.BlockSpec((LOCAL, 1, NX, NY), lambda z: (0, z, 0, 0)),
        ],
        out_specs=[whole, whole],
        out_shape=[jax.ShapeDtypeStruct((64, PIECE, 128), t) for t in (F32, BF16)],
        scratch_shapes=[
            pltpu.VMEM((8, DEPTH), F32),
            pltpu.VMEM((NS * 8 + 8, DEPTH), BF16),
            pltpu.VMEM((8 * LOCAL * PITCH + 8, 128), F32),
            pltpu.VMEM(((NX + 4) * LOCAL + 16, 128), BF16),
            pltpu.VMEM((14 * NX * PACE, 128), F32),
            pltpu.VMEM((EXT * NX, 128), F32),
        ],
        compiler_params=pltpu.CompilerParams(vmem_limit_bytes=48 << 20),
        cost_estimate=pl.CostEstimate(flops=20_000_000_000, bytes_accessed=16_000_000, transcendentals=0),
        name="moments",
    )(idx, prop, par, state)


def gather_kernel(got_ref, temp_ref, bulk_ref, label_ref, own_ref, known_ref, edge_ref, sums_ref, total):
    lane = lane_iota((8, 128))
    group = lane // 32
    inner = (lane % 32 >= 8) & (lane % 32 < 24)
    for s in range(8):
        for d in range(DEPTHS):
            value = got_ref[8 * s, 8 * d : 8 * d + 8, :].astype(F32)
            for q in range(1, 8):
                value = value + got_ref[8 * s + q, 8 * d : 8 * d + 8, :].astype(F32)
            total[s * DEPTHS + d] = value

    sums = total[0] + pltpu.roll(total[1], 80, 1)
    sums_ref[...] = sums + pltpu.roll(sums, 4, 0)

    def layer(s, f, zo, quarter):
        depth = f * EXT + zo
        turn = (32 * quarter + 8 - 16 * (depth % 8)) % 128
        value = total[s * DEPTHS + depth // 8]
        return pltpu.roll(value, turn, 1) if turn else value

    for f in range(6):
        reach = 1 if f == 0 else 2
        for zz in range(16):
            value = None
            for quarter in range(4):
                z = quarter * 16 + zz
                s = z // 8
                part = layer(s, f, z % 8 + 2, quarter)
                if z % 8 < reach and s > 0:
                    part = part + layer(s - 1, f, z % 8 + 10, quarter)
                if z % 8 > 7 - reach and s < 7:
                    part = part + layer(s + 1, f, z % 8 - 6, quarter)
                value = part if quarter == 0 else jnp.where(group >= quarter, part, value)
            own_ref[f, zz] = value

    wide_group = lane_iota((16, 128)) // 32

    def block_of(n, read):
        cells = jnp.concatenate([read(pl.ds(y, 16, stride=8)) for y in range(8)], axis=0).T
        for y in range(8):
            value = None
            for quarter in range(4):
                turn = (32 * quarter + 8 - 16 * y) % 128
                part = cells[16 * quarter : 16 * quarter + 16]
                part = pltpu.roll(part, turn, 1) if turn else part
                value = part if quarter == 0 else jnp.where(wide_group >= quarter, part, value)
            known_ref[n, pl.ds(y, 16, stride=8), :] = value

    block_of(0, lambda rows: temp_ref[rows, :])
    block_of(1, lambda rows: bulk_ref[rows, :] * jnp.where(label_ref[rows, :] == 1, 0.1, 1.0))

    for n in range(7):

        def cells(zz):
            if n < 5:
                return own_ref[n, zz]
            return known_ref[n - 5, 8 * zz : 8 * zz + 8, :]

        for h in range(8):
            packed = jnp.where(inner, cells(2 * h), pltpu.roll(cells(2 * h + 1), 16, 1))
            edge_ref[(n * 8 + h) * 8 : (n * 8 + h) * 8 + 8, :] = packed.astype(BF16)


def gathered(got, temp, bulk, label):
    flat = [value.reshape(128, NZ) for value in (temp, bulk, label)]
    return pl.pallas_call(
        gather_kernel,
        out_shape=[
            jax.ShapeDtypeStruct((6, 16, 8, 128), F32),
            jax.ShapeDtypeStruct((2, 128, 128), F32),
            jax.ShapeDtypeStruct((7 * 64, 128), BF16),
            jax.ShapeDtypeStruct((8, 128), F32),
        ],
        scratch_shapes=[pltpu.VMEM((8 * DEPTHS, 8, 128), F32)],
        name="gather",
    )(got, *flat)


def widen_kernel(own_ref, known_ref, west_ref, east_ref, wide_ref, halo_ref):
    part = lane_iota((8, 128)) % 32
    for n in range(7):
        for zz in range(16):
            at = (n * 8 + zz // 2) * 8
            west = pltpu.roll(west_ref[at : at + 8, :].astype(F32), 96 if zz % 2 else 112, 1)
            east = east_ref[at : at + 8, :].astype(F32)
            if zz % 2 == 0:
                east = pltpu.roll(east, 16, 1)
            own = own_ref[n, zz] if n < 5 else known_ref[n - 5, 8 * zz : 8 * zz + 8, :]
            value = jnp.where(part < 8, west, jnp.where(part < 24, own, east))
            wide_ref[n, zz] = value
            halo_ref[(n * 16 + zz) * 8 : (n * 16 + zz) * 8 + 8, :] = value.astype(BF16)


def widened(own, known, west, east):
    return pl.pallas_call(
        widen_kernel,
        out_shape=[
            jax.ShapeDtypeStruct((7, 16, 8, 128), F32),
            jax.ShapeDtypeStruct((7 * 128, 128), BF16),
        ],
        name="widen",
    )(own, known, west, east)


def solve_kernel(
    idx_ref, sums_ref, own_ref, south_hbm, north_hbm, wide_ref, temp_ref, flux_ref, halo, lines, sems
):
    copies = [
        pltpu.make_async_copy(src, halo.at[n], sems.at[n]) for n, src in enumerate((south_hbm, north_hbm))
    ]
    for copy in copies:
        copy.start()
    for copy in copies:
        copy.wait()
    shape = (16, 24, 128)
    lane = lane_iota((1, 24, 128))
    x = lane % 32 + (idx_ref[0] * 16 - 8)
    y = lax.broadcasted_iota(jnp.int32, (1, 24, 128), 1) + (idx_ref[1] * 8 - 8)
    inside = jnp.where((x >= 0) & (x < NX) & (y >= 0) & (y < NY), 1.0, 0.0)
    group = lane_iota((1, 24, 128)) // 32

    def wide(own, f):
        rows = slice(f * 128, f * 128 + 128)
        south = halo[0, rows, :].astype(F32).reshape(16, 8, 128)
        north = halo[1, rows, :].astype(F32).reshape(16, 8, 128)
        return jnp.concatenate([south, own, north], axis=1)

    def field(f):
        return wide(wide_ref[f], f)

    def known(n):
        return wide(wide_ref[5 + n], 5 + n)

    def east(v):
        return pltpu.roll(v, 127, 2)

    def west(v):
        return pltpu.roll(v, 1, 2)

    def north(v):
        return jnp.concatenate([v[:, 1:], jnp.zeros((16, 1, 128), F32)], axis=1)

    def south(v):
        return jnp.concatenate([jnp.zeros((16, 1, 128), F32), v[:, :-1]], axis=1)

    def above(v):
        edge = jnp.where(group < 3, pltpu.roll(v[0:1], 96, 2), 0.0)
        return jnp.concatenate([v[1:], edge], axis=0)

    def below(v):
        edge = jnp.where(group > 0, pltpu.roll(v[15:16], 32, 2), 0.0)
        return jnp.concatenate([edge, v[:-1]], axis=0)

    total_scalar = sums_ref[0, 8]
    total = jnp.full((1, 24, 128), total_scalar, F32)
    theta = total + 6.0
    sigma = theta / 6.0
    kappa = known(1)

    def face(a, b):
        summed = a + b
        positive = summed > 0.0
        return jnp.where(positive, 2.0 * a * b / jnp.where(positive, summed, 1.0), 0.0)

    face_e = face(kappa, east(kappa))
    face_n = face(kappa, north(kappa))
    face_u = face(kappa, above(kappa))
    face_w = west(face_e)
    face_s = south(face_n)
    face_d = below(face_u)

    def operator(v):
        out = face_e * (east(v) - v) + face_w * (west(v) - v)
        out = out + face_n * (north(v) - v) + face_s * (south(v) - v)
        out = out + face_u * (above(v) - v) + face_d * (below(v) - v)
        return total * v - out

    def chebyshev(rhs):
        rho = 1.0 / sigma
        residual = rhs
        direction = rhs / theta
        correction = direction
        for sweep in range(SWEEPS - 1):
            residual = residual - operator(direction)
            rho_next = 1.0 / (2.0 * sigma - rho)
            direction = rho_next * rho * direction + 2.0 * rho_next / 6.0 * residual
            rho = rho_next
            correction = correction + direction
        return correction

    temp = known(0)
    moved = (temp, west(temp), east(temp), south(temp), north(temp), below(temp), above(temp))
    gain = [sums_ref[k, 7] for k in range(4)]
    rhs = 0.5 * (
        gain[1] * (moved[2] - moved[1]) + gain[2] * (moved[4] - moved[3]) + gain[3] * (moved[6] - moved[5])
    )
    rhs = -(field(1) + rhs)
    once = (field(0) + gain[0] * temp) / total + chebyshev(rhs)

    def second(k, part):
        value = part + gain[k] * once
        for s in range(7):
            value = value + sums_ref[k, s] * moved[s]
        return value

    flux = [second(k, field(k + 1)) * inside for k in (1, 2, 3)]
    own = own_ref[5]
    energy = second(0, jnp.concatenate([own, own, own], axis=1))
    rhs = -0.5 * (
        (east(flux[0]) - west(flux[0])) + (north(flux[1]) - south(flux[1])) + (above(flux[2]) - below(flux[2]))
    )
    twice = energy / total + chebyshev(rhs)
    quarter = lane_iota((16, 128)) // 16

    def write(n, value, store):
        for zz in range(16):
            lines[n, zz * PACE : zz * PACE + 8, :] = value[zz, 8:16]
        rows = [lines[n, pl.ds(y, 16, stride=PACE), :] for y in range(8)]
        turned = jnp.concatenate(rows, axis=0).T
        for y in range(8):
            out = None
            for q in range(4):
                part = turned[32 * q + 8 : 32 * q + 24]
                move = (16 * (q - y)) % 128
                part = pltpu.roll(part, move, 1) if move else part
                out = part if q == 0 else jnp.where(quarter >= q, part, out)
            store(y, out[:, :64])

    def store_temp(y, out):
        temp_ref[pl.ds(y, 16, stride=8), :] = out

    write(0, twice, store_temp)
    for n in range(3):

        def store_flux(y, out, n=n):
            flux_ref[n, pl.ds(y, 16, stride=8), :] = out

        write(n + 1, flux[n], store_flux)


def solved(idx, sums, own, south, north, wide):
    vmem = pl.BlockSpec(memory_space=pltpu.VMEM)
    smem = pl.BlockSpec(memory_space=pltpu.SMEM)
    return pl.pallas_call(
        solve_kernel,
        in_specs=[smem, smem, vmem] + [pl.BlockSpec(memory_space=pl.ANY)] * 2 + [vmem],
        out_specs=[vmem, vmem],
        out_shape=[
            jax.ShapeDtypeStruct((128, 64), F32),
            jax.ShapeDtypeStruct((3, 128, 64), F32),
        ],
        scratch_shapes=[
            pltpu.VMEM((2, 7 * 128, 128), BF16),
            pltpu.VMEM((4, 16 * PACE, 128), F32),
            pltpu.SemaphoreType.DMA((2,)),
        ],
        compiler_params=pltpu.CompilerParams(vmem_limit_bytes=48 << 20),
        name="solve",
    )(idx, sums, own, south, north, wide)


LINE = ("zy", "core")


def both_ways(value, axis, count):
    ahead = [(i, i + 1) for i in range(count - 1)]
    behind = [(i + 1, i) for i in range(count - 1)]
    return lax.ppermute(value, axis, ahead), lax.ppermute(value, axis, behind)


def per_device(
    excess_phonon_enthalpy,
    thermal_offset,
    state_specific_warmth_scaled,
    scattering_lifetimes,
    state_polarization_label,
    state_orientation_label,
    polarization_propagation_rate,
    thermal_conductance_bulk,
    substance_label,
):
    space = lax.axis_index("space")
    core = lax.axis_index("core")
    line = lax.axis_index("zy") * 2 + core
    table = jnp.stack(
        [
            state_polarization_label.astype(F32),
            state_orientation_label.astype(F32),
            state_specific_warmth_scaled,
            scattering_lifetimes,
        ]
    )
    keep, send = moments(
        jnp.stack([space, core]).astype(jnp.int32),
        polarization_propagation_rate,
        table,
        excess_phonon_enthalpy,
    )
    received = lax.ppermute(send, "core", [(0, 1), (1, 0)])
    paired = (keep + received.astype(F32)).astype(BF16)
    got = lax.all_to_all(paired, ("space", "zy"), 0, 0, tiled=True)
    own, known, edge, sums = gathered(got, thermal_offset, thermal_conductance_bulk, substance_label)
    west, east = both_ways(edge, "space", 8)
    wide, halo = widened(own, known, west, east)
    south, north = both_ways(halo, LINE, 16)
    temp, flux = solved(jnp.stack([space, line]).astype(jnp.int32), sums, own, south, north, wide)
    return temp.reshape(16, 8, 64), flux.reshape(3, 16, 8, 64)


def solution(mesh):
    parts = Mesh(mesh.devices.reshape(8, 8, 2), ("space", "zy", "core"))
    modes = P(LINE)
    block = P("space", LINE, None)
    return jax.shard_map(
        per_device,
        mesh=parts,
        in_specs=(P(LINE, "space", None, None), block, modes, modes, modes, modes, P(), block, block),
        out_specs=(block, P(None, "space", LINE, None)),
        check_vma=False,
    )
```

```python
import math

import jax
import jax.numpy as jnp
from jax import lax
from jax.experimental import pallas as pl
from jax.experimental.pallas import tpu as pltpu
from jax.sharding import Mesh, PartitionSpec as P

SWEEPS = 4
STEP = 0.25
MODES = 768
LOCAL = 48
SLAB = 8
NX = 128
NY = 128
NZ = 64
WIN = 5 * LOCAL
DEPTH = 256
EXT = 12
PITCH = 17
PACE = 9
LAYERS = 6 * EXT
DEPTHS = LAYERS // 8
PIECE = DEPTHS * 8
F32 = jnp.float32
BF16 = jnp.bfloat16

SHIFTS = (
    (0, 0), (1, 0), (-1, 0), (2, 0), (-2, 0),
    (0, 1), (1, 1), (-1, 1),
    (0, -1), (1, -1), (-1, -1),
    (0, 2), (0, -2),
)
NS = len(SHIFTS)
BY_Z = tuple(
    (sz, tuple((sy, n) for n, (sy, z) in enumerate(SHIFTS) if z == sz)) for sz in (-2, -1, 0, 1, 2)
)


def lane_iota(shape):
    return lax.broadcasted_iota(jnp.int32, shape, len(shape) - 1)


def mode_rows(table):
    labels = table[0:1, :]
    branch = sum(jnp.where(labels >= 16.0 * b, 1.0, 0.0) for b in range(1, 6))
    orient = labels - 16.0 * branch
    cap = table[1:2, :] / float(MODES)
    rate = 1.0 / table[2:3, :]
    speed = jnp.zeros_like(branch)
    for b in range(6):
        speed = speed + jnp.where(branch == float(b), table[3:4, b : b + 1], 0.0)
    polar = jnp.where(orient >= 4.0, 1.0, 0.0) + jnp.where(orient >= 8.0, 1.0, 0.0)
    polar = polar + jnp.where(orient >= 12.0, 1.0, 0.0)
    turn = orient - 4.0 * polar
    cosine = (2.0 * polar + 1.0) * 0.25 - 1.0
    sine = jnp.sqrt(1.0 - cosine * cosine)
    half = math.sqrt(0.5)
    east = jnp.where((turn == 0.0) | (turn == 3.0), half, -half)
    north = jnp.where(turn < 2.0, half, -half)
    return speed * sine * east, speed * sine * north, speed * cosine, rate, cap


def step_terms(vx, vy, vz, rate):
    cx, cy, cz = (STEP * jnp.abs(v) for v in (vx, vy, vz))
    c0 = 1.0 - cx - cy - cz - STEP * rate
    one = (((0, 0, 0), c0), ((1, 0, 0), cx), ((0, 1, 0), cy), ((0, 0, 1), cz))
    two = (
        ((0, 0, 0), c0 * c0),
        ((1, 0, 0), 2.0 * c0 * cx),
        ((0, 1, 0), 2.0 * c0 * cy),
        ((0, 0, 1), 2.0 * c0 * cz),
        ((2, 0, 0), cx * cx),
        ((0, 2, 0), cy * cy),
        ((0, 0, 2), cz * cz),
        ((1, 1, 0), 2.0 * cx * cy),
        ((1, 0, 1), 2.0 * cx * cz),
        ((0, 1, 1), 2.0 * cy * cz),
    )
    return one, two


def fields_on_rows(vx, vy, vz, rate):
    lanes = rate.shape[1]
    row = lax.broadcasted_iota(jnp.int32, (8, lanes), 0) % 4
    full = [jnp.broadcast_to(v, (8, lanes)) for v in (rate, vx, vy, vz)]
    return jnp.where(
        row == 0, full[0], jnp.where(row == 1, full[1], jnp.where(row == 2, full[2], full[3]))
    )


def build_tables(par_ref, par5, coef):
    par5[...] = jnp.ones(par5.shape, F32)
    for n in range(4):
        for o in range(5):
            par5[n : n + 1, o * LOCAL : (o + 1) * LOCAL] = par_ref[:, n * LOCAL : (n + 1) * LOCAL]
    vx, vy, vz, rate, _ = mode_rows(par5)
    one, two = step_terms(vx, vy, vz, rate)
    weights = fields_on_rows(vx, vy, vz, rate)
    lane = lane_iota((1, DEPTH))
    offset = -2.0 + sum(jnp.where(lane >= o * LOCAL, 1.0, 0.0) for o in range(1, 5))
    inside = lane < WIN
    dx, dy, dz = (jnp.where(v > 0.0, 1.0, -1.0) for v in (vx, vy, vz))
    upper = lax.broadcasted_iota(jnp.int32, (8, DEPTH), 0) < 4

    def total(terms, sy, sz):
        out = jnp.zeros((1, DEPTH), F32)
        for (ax, ay, az), value in terms:
            if ay != abs(sy) or az != abs(sz):
                continue
            hit = inside & (offset == -float(ax) * dx)
            if ay:
                hit = hit & (dy * float(ay) == float(sy))
            if az:
                hit = hit & (dz * float(az) == float(sz))
            out = out + jnp.where(hit, value, 0.0)
        return jnp.broadcast_to(out, (8, DEPTH))

    parts = [
        weights * jnp.where(upper, total(one, sy, sz), total(two, sy, sz)) for sy, sz in SHIFTS
    ]
    rest = parts[0] - parts[0].astype(BF16).astype(F32)
    coef[...] = jnp.concatenate(parts + [rest], axis=0).astype(BF16)


def mode_sums(par5, core):
    vx, vy, vz, rate, cap = mode_rows(par5)
    one, _ = step_terms(vx, vy, vz, rate)
    weights = fields_on_rows(vx, vy, vz, rate)
    gain = STEP * rate * cap
    columns = [weights * gain * one[0][1]]
    for ((ax, ay, az), value), v in zip(one[1:], (vx, vy, vz)):
        for sign in (1.0, -1.0):
            columns.append(weights * gain * jnp.where(v * sign > 0.0, value, 0.0))
    columns.append(weights * gain)
    columns.append(jnp.broadcast_to(cap * rate, weights.shape))
    mine = lane_iota(weights.shape) < LOCAL
    lane = lane_iota((8, 128))
    sums = jnp.zeros((8, 128), F32)
    for n, column in enumerate(columns):
        sums = jnp.where(lane == n, jnp.sum(jnp.where(mine, column, 0.0), axis=1, keepdims=True), sums)
    row = lax.broadcasted_iota(jnp.int32, (8, 128), 0)
    sums = jnp.where((row // 4) == core, sums, 0.0)
    high = sums.astype(BF16).astype(F32)
    return high, pltpu.roll(sums - high, 48, 1)


def moments_kernel(idx_ref, par_ref, e_ref, keep_ref, send_ref, par5, coef, spread, turned, acc, drift):
    z = pl.program_id(0)
    space = idx_ref[0]
    core = idx_ref[1]
    LAYER = NX * PACE

    @pl.when(z == 0)
    def _():
        build_tables(par_ref, par5, coef)
        turned[0 : 2 * LOCAL, :] = jnp.zeros((2 * LOCAL, 128), BF16)
        turned[(NX + 2) * LOCAL :, :] = jnp.zeros((2 * LOCAL + 16, 128), BF16)

        @pl.loop(0, 5 * LAYER // 64)
        def _(r):
            acc[pl.ds(pl.multiple_of(r * 64, 64), 64), :] = jnp.zeros((64, 128), F32)

        acc[13 * LAYER : 14 * LAYER, :] = jnp.zeros((LAYER, 128), F32)

    def turn(c):
        for m in range(LOCAL):
            at = (c * LOCAL + m) * PITCH
            spread[at : at + 16, :] = e_ref[m, 0, 16 * c : 16 * c + 16, :].astype(F32)
        for xx in range(16):
            rows = spread[pl.ds(c * LOCAL * PITCH + xx, LOCAL, stride=PITCH), :].astype(BF16)
            at = (16 * c + xx + 2) * LOCAL
            turned[at : at + LOCAL, :] = rows

    lane = lane_iota((8, 128))

    def moved(value, sy):
        if sy == 0:
            return value
        rolled = pltpu.roll(value, sy % 128, 1)
        return jnp.where(lane >= sy if sy > 0 else lane < 128 + sy, rolled, 0.0)

    def one_pair(x):
            first = turned[x * LOCAL : x * LOCAL + DEPTH, :]
            second = turned[(x + 1) * LOCAL : (x + 1) * LOCAL + DEPTH, :]
            block = jnp.concatenate([first, second], axis=1)
            out = jnp.dot(coef[...], block, preferred_element_type=F32)
            for half in range(2):
                for sz, members in BY_Z:
                    total = None
                    for sy, n in members:
                        part = moved(out[8 * n : 8 * n + 8, 128 * half : 128 * half + 128], sy)
                        if n == 0:
                            part = part + out[8 * NS :, 128 * half : 128 * half + 128]
                        total = part if total is None else total + part
                    at = (z + 3 + sz) * LAYER + (x + half) * PACE
                    if sz == 2:
                        acc[pl.ds(at, 8), :] = total
                    else:
                        acc[pl.ds(at, 8), :] += total

    CHUNKS = NX // 16
    turn(0)
    for c in range(CHUNKS):
        if c + 1 < CHUNKS:
            turn(c + 1)
        for x in range(16 * c, 16 * c + 16, 2):
            one_pair(x)

    @pl.when(z == SLAB - 1)
    def _():
        @pl.when(space == 0)
        def _():
            acc[LAYER : 3 * LAYER, :] = jnp.zeros((2 * LAYER, 128), F32)

        @pl.when(space == 7)
        def _():
            acc[11 * LAYER : 13 * LAYER, :] = jnp.zeros((2 * LAYER, 128), F32)

        row = lax.broadcasted_iota(jnp.int32, (NX, 128), 0)
        col = lane_iota((NX, 128))

        def layer(zo, field, shift=0):
            return acc[pl.ds((zo + 1) * LAYER + field + PACE * shift, NX, stride=PACE), :]

        def divergence(zo):
            east = jnp.where(row < NX - 1, layer(zo, 1, 1), 0.0)
            west = jnp.where(row > 0, layer(zo, 1, -1), 0.0)
            along_y = layer(zo, 2)
            north = jnp.where(col < 127, pltpu.roll(along_y, 127, 1), 0.0)
            south = jnp.where(col > 0, pltpu.roll(along_y, 1, 1), 0.0)
            up = layer(zo + 1, 3)
            down = layer(zo - 1, 3)
            return 0.5 * ((east - west) + (north - south) + (up - down))

        for zo in range(EXT):
            drift[zo * NX : zo * NX + NX, :] = divergence(zo)
        rows = (0, None, 5, 6, 7, 4)
        extras = mode_sums(par5, core)

        def strip(depth, i):
            f, zo = divmod(depth, EXT)
            if rows[f] is None:
                return drift[zo * NX + 16 * i : zo * NX + 16 * i + 16, :]
            return acc[pl.ds((zo + 1) * LAYER + rows[f] + 16 * i * PACE, 16, stride=PACE), :]

        for d in range(DEPTHS):
            for i in range(8):
                tile = jnp.concatenate([strip(8 * d + low, i) for low in range(8)], axis=0).T
                for p in range(8):
                    first, second = tile[16 * p : 16 * p + 8], tile[16 * p + 8 : 16 * p + 16]
                    kept = jnp.where(core == 0, first, second)
                    sent = jnp.where(core == 0, second, first)
                    if d < 2:
                        kept = kept + extras[d]
                        sent = sent + extras[d]
                    keep_ref[8 * i + p, 8 * d : 8 * d + 8, :] = kept
                    send_ref[8 * i + p, 8 * d : 8 * d + 8, :] = sent.astype(BF16)


def moments(idx, table, state):
    whole = pl.BlockSpec((64, PIECE, 128), lambda z: (0, 0, 0))
    return pl.pallas_call(
        moments_kernel,
        grid=(SLAB,),
        in_specs=[
            pl.BlockSpec(memory_space=pltpu.SMEM),
            pl.BlockSpec((1, 4 * LOCAL), lambda z: (0, 0)),
            pl.BlockSpec((LOCAL, 1, NX, NY), lambda z: (0, z, 0, 0)),
        ],
        out_specs=[whole, whole],
        out_shape=[jax.ShapeDtypeStruct((64, PIECE, 128), t) for t in (F32, BF16)],
        scratch_shapes=[
            pltpu.VMEM((8, DEPTH), F32),
            pltpu.VMEM((NS * 8 + 8, DEPTH), BF16),
            pltpu.VMEM((8 * LOCAL * PITCH + 8, 128), F32),
            pltpu.VMEM(((NX + 4) * LOCAL + 16, 128), BF16),
            pltpu.VMEM((14 * NX * PACE, 128), F32),
            pltpu.VMEM((EXT * NX, 128), F32),
        ],
        compiler_params=pltpu.CompilerParams(vmem_limit_bytes=48 << 20),
        cost_estimate=pl.CostEstimate(flops=20_000_000_000, bytes_accessed=16_000_000, transcendentals=0),
        name="moments",
    )(idx, table, state)


def gather_kernel(
    got_ref, temp_ref, bulk_ref, label_ref, own_ref, known_ref, east_ref, west_ref, sums_ref, total
):
    lane = lane_iota((8, 128))
    group = lane // 32
    eighth = (lane % 32) // 8
    for s in range(8):
        for d in range(DEPTHS):
            value = got_ref[8 * s, 8 * d : 8 * d + 8, :].astype(F32)
            for q in range(1, 8):
                value = value + got_ref[8 * s + q, 8 * d : 8 * d + 8, :].astype(F32)
            total[s * DEPTHS + d] = value

    sums = total[0] + pltpu.roll(total[1], 80, 1)
    sums_ref[...] = sums + pltpu.roll(sums, 4, 0)

    def layer(s, f, zo, quarter):
        depth = f * EXT + zo
        turn = (32 * quarter + 8 - 16 * (depth % 8)) % 128
        value = total[s * DEPTHS + depth // 8]
        return pltpu.roll(value, turn, 1) if turn else value

    for f in range(6):
        reach = 1 if f == 0 else 2
        for zz in range(16):
            value = None
            for quarter in range(4):
                z = quarter * 16 + zz
                s = z // 8
                part = layer(s, f, z % 8 + 2, quarter)
                if z % 8 < reach and s > 0:
                    part = part + layer(s - 1, f, z % 8 + 10, quarter)
                if z % 8 > 7 - reach and s < 7:
                    part = part + layer(s + 1, f, z % 8 - 6, quarter)
                value = part if quarter == 0 else jnp.where(group >= quarter, part, value)
            own_ref[f, zz] = value

    wide_group = lane_iota((16, 128)) // 32

    def block_of(n, read):
        cells = jnp.concatenate([read(pl.ds(y, 16, stride=8)) for y in range(8)], axis=0).T
        for y in range(8):
            value = None
            for quarter in range(4):
                turn = (32 * quarter + 8 - 16 * y) % 128
                part = cells[16 * quarter : 16 * quarter + 16]
                part = pltpu.roll(part, turn, 1) if turn else part
                value = part if quarter == 0 else jnp.where(wide_group >= quarter, part, value)
            known_ref[n, pl.ds(y, 16, stride=8), :] = value

    block_of(0, lambda rows: temp_ref[rows, :])
    block_of(1, lambda rows: bulk_ref[rows, :] * jnp.where(label_ref[rows, :] == 1, 0.1, 1.0))

    for n in range(7):

        def cells(zz):
            if n < 5:
                return own_ref[n, zz]
            return known_ref[n - 5, 8 * zz : 8 * zz + 8, :]

        for h in range(4):
            rows = slice((n * 4 + h) * 8, (n * 4 + h) * 8 + 8)
            for ref, first in ((east_ref, 16), (west_ref, 8)):
                packed = None
                for k in range(4):
                    turn = (8 * k - first) % 128
                    value = cells(4 * h + k)
                    value = pltpu.roll(value, turn, 1) if turn else value
                    packed = value if k == 0 else jnp.where(eighth == k, value, packed)
                ref[rows, :] = packed.astype(BF16)


def gathered(got, temp, bulk, label):
    flat = [value.reshape(128, NZ) for value in (temp, bulk, label)]
    return pl.pallas_call(
        gather_kernel,
        out_shape=[
            jax.ShapeDtypeStruct((6, 16, 8, 128), F32),
            jax.ShapeDtypeStruct((2, 128, 128), F32),
            jax.ShapeDtypeStruct((7 * 32, 128), BF16),
            jax.ShapeDtypeStruct((7 * 32, 128), BF16),
            jax.ShapeDtypeStruct((8, 128), F32),
        ],
        scratch_shapes=[pltpu.VMEM((8 * DEPTHS, 8, 128), F32)],
        name="gather",
    )(got, *flat)


FULL = (1, 5, 6)
HALVES = ((0, 2), (3, 4))
HALO = (len(FULL) + len(HALVES)) * 128


def widen_kernel(idx_ref, own_ref, known_ref, west_ref, east_ref, wide_ref, cross_ref, partner_ref):
    part = lane_iota((8, 128)) % 32
    row = lax.broadcasted_iota(jnp.int32, (8, 128), 0)
    core = idx_ref[1]

    def cells(n, zz):
        at = (n * 4 + zz // 4) * 8
        k = zz % 4
        west = west_ref[at : at + 8, :].astype(F32)
        west = pltpu.roll(west, 128 - 8 * k, 1) if k else west
        east = east_ref[at : at + 8, :].astype(F32)
        east = pltpu.roll(east, 24 - 8 * k, 1) if k < 3 else east
        own = own_ref[n, zz] if n < 5 else known_ref[n - 5, 8 * zz : 8 * zz + 8, :]
        value = jnp.where(part < 8, west, jnp.where(part < 24, own, east))
        wide_ref[n, zz] = value
        return value

    for zz in range(16):
        wide_ref[7, zz] = own_ref[5, zz]
        for u, n in enumerate(FULL):
            value = cells(n, zz).astype(BF16)
            at = (u * 16 + zz) * 8
            cross_ref[at : at + 8, :] = value
            partner_ref[at : at + 8, :] = value
        for u, (n, m) in enumerate(HALVES):
            value = cells(n, zz)
            other = pltpu.roll(cells(m, zz), 4, 0)
            southward = jnp.where(row < 4, value, other)
            northward = jnp.where(row < 4, other, value)
            at = ((len(FULL) + u) * 16 + zz) * 8
            cross_ref[at : at + 8, :] = jnp.where(core == 0, southward, northward).astype(BF16)
            partner_ref[at : at + 8, :] = jnp.where(core == 0, northward, southward).astype(BF16)


def widened(idx, own, known, west, east):
    vmem = pl.BlockSpec(memory_space=pltpu.VMEM)
    return pl.pallas_call(
        widen_kernel,
        in_specs=[pl.BlockSpec(memory_space=pltpu.SMEM)] + [vmem] * 4,
        out_shape=[
            jax.ShapeDtypeStruct((8, 16, 8, 128), F32),
            jax.ShapeDtypeStruct((HALO, 128), BF16),
            jax.ShapeDtypeStruct((HALO, 128), BF16),
        ],
        name="widen",
    )(idx, own, known, west, east)


def solve_kernel(idx_ref, sums_vmem, cross_ref, partner_ref, wide_ref, temp_ref, flux_ref, lines, sums_ref, sem):
    copy = pltpu.make_async_copy(sums_vmem, sums_ref, sem)
    copy.start()
    shape = (16, 24, 128)
    lane = lane_iota((1, 24, 128))
    x = lane % 32 + (idx_ref[0] * 16 - 8)
    y = lax.broadcasted_iota(jnp.int32, (1, 24, 128), 1) + (idx_ref[1] * 8 - 8)
    inside = jnp.where((x >= 0) & (x < NX) & (y >= 0) & (y < NY), 1.0, 0.0)
    group = lane_iota((1, 24, 128)) // 32

    def sent(ref, f):
        if f in FULL:
            u = FULL.index(f)
            return ref[u * 128 : u * 128 + 128, :].astype(F32).reshape(16, 8, 128)
        u, second = next((u, pair.index(f)) for u, pair in enumerate(HALVES) if f in pair)
        at = (len(FULL) + u) * 128
        value = ref[at : at + 128, :].astype(F32).reshape(16, 8, 128)
        return pltpu.roll(value, 4, 1) if second else value

    def field(f):
        cross = sent(cross_ref, f)
        partner = sent(partner_ref, f)
        first = idx_ref[2] == 0
        south = jnp.where(first, cross, partner)
        north = jnp.where(first, partner, cross)
        return jnp.concatenate([south, wide_ref[f], north], axis=1)

    def known(n):
        return field(5 + n)

    def east(v):
        return pltpu.roll(v, 127, 2)

    def west(v):
        return pltpu.roll(v, 1, 2)

    def north(v):
        return jnp.concatenate([v[:, 1:], jnp.zeros((16, 1, 128), F32)], axis=1)

    def south(v):
        return jnp.concatenate([jnp.zeros((16, 1, 128), F32), v[:, :-1]], axis=1)

    def above(v):
        edge = jnp.where(group < 3, pltpu.roll(v[0:1], 96, 2), 0.0)
        return jnp.concatenate([v[1:], edge], axis=0)

    def below(v):
        edge = jnp.where(group > 0, pltpu.roll(v[15:16], 32, 2), 0.0)
        return jnp.concatenate([edge, v[:-1]], axis=0)

    kappa = known(1)

    def face(a, b):
        summed = a + b
        positive = summed > 0.0
        return jnp.where(positive, 2.0 * a * b / jnp.where(positive, summed, 1.0), 0.0)

    face_e = face(kappa, east(kappa))
    face_n = face(kappa, north(kappa))
    face_u = face(kappa, above(kappa))
    face_w = west(face_e)
    face_s = south(face_n)
    face_d = below(face_u)

    copy.wait()
    total = jnp.full((1, 24, 128), sums_ref[0, 8], F32)
    theta = total + 6.0
    sigma = theta / 6.0

    def operator(v):
        out = face_e * (east(v) - v) + face_w * (west(v) - v)
        out = out + face_n * (north(v) - v) + face_s * (south(v) - v)
        out = out + face_u * (above(v) - v) + face_d * (below(v) - v)
        return total * v - out

    def chebyshev(rhs):
        rho = 1.0 / sigma
        residual = rhs
        direction = rhs / theta
        correction = direction
        for sweep in range(SWEEPS - 1):
            residual = residual - operator(direction)
            rho_next = 1.0 / (2.0 * sigma - rho)
            direction = rho_next * rho * direction + 2.0 * rho_next / 6.0 * residual
            rho = rho_next
            correction = correction + direction
        return correction

    temp = known(0)
    moved = (temp, west(temp), east(temp), south(temp), north(temp), below(temp), above(temp))
    gain = [sums_ref[k, 7] for k in range(4)]
    rhs = 0.5 * (
        gain[1] * (moved[2] - moved[1]) + gain[2] * (moved[4] - moved[3]) + gain[3] * (moved[6] - moved[5])
    )
    rhs = -(field(1) + rhs)
    once = (field(0) + gain[0] * temp) / total + chebyshev(rhs)

    def second(k, part):
        value = part + gain[k] * once
        for s in range(7):
            value = value + sums_ref[k, s] * moved[s]
        return value

    flux = [second(k, field(k + 1)) * inside for k in (1, 2, 3)]
    own = wide_ref[7]
    energy = second(0, jnp.concatenate([own, own, own], axis=1))
    rhs = -0.5 * (
        (east(flux[0]) - west(flux[0])) + (north(flux[1]) - south(flux[1])) + (above(flux[2]) - below(flux[2]))
    )
    twice = energy / total + chebyshev(rhs)
    quarter = lane_iota((16, 128)) // 16

    def write(n, value, store):
        for zz in range(16):
            lines[n, zz * PACE : zz * PACE + 8, :] = value[zz, 8:16]
        rows = [lines[n, pl.ds(y, 16, stride=PACE), :] for y in range(8)]
        turned = jnp.concatenate(rows, axis=0).T
        for y in range(8):
            out = None
            for q in range(4):
                part = turned[32 * q + 8 : 32 * q + 24]
                move = (16 * (q - y)) % 128
                part = pltpu.roll(part, move, 1) if move else part
                out = part if q == 0 else jnp.where(quarter >= q, part, out)
            store(y, out[:, :64])

    def store_temp(y, out):
        temp_ref[pl.ds(y, 16, stride=8), :] = out

    write(0, twice, store_temp)
    for n in range(3):

        def store_flux(y, out, n=n):
            flux_ref[n, pl.ds(y, 16, stride=8), :] = out

        write(n + 1, flux[n], store_flux)


def solved(idx, sums, cross, partner, wide):
    vmem = pl.BlockSpec(memory_space=pltpu.VMEM)
    return pl.pallas_call(
        solve_kernel,
        in_specs=[pl.BlockSpec(memory_space=pltpu.SMEM)] + [vmem] * 4,
        out_specs=[vmem, vmem],
        out_shape=[
            jax.ShapeDtypeStruct((128, 64), F32),
            jax.ShapeDtypeStruct((3, 128, 64), F32),
        ],
        scratch_shapes=[
            pltpu.VMEM((4, 16 * PACE, 128), F32),
            pltpu.SMEM((8, 128), F32),
            pltpu.SemaphoreType.DMA(()),
        ],
        compiler_params=pltpu.CompilerParams(vmem_limit_bytes=48 << 20),
        name="solve",
    )(idx, sums, cross, partner, wide)


LINE = ("zy", "core")


def per_device(
    excess_phonon_enthalpy,
    thermal_offset,
    state_specific_warmth_scaled,
    scattering_lifetimes,
    state_polarization_label,
    state_orientation_label,
    polarization_propagation_rate,
    thermal_conductance_bulk,
    substance_label,
):
    space = lax.axis_index("space")
    core = lax.axis_index("core")
    line = lax.axis_index("zy") * 2 + core
    idx = jnp.stack([space, core]).astype(jnp.int32)
    labels = state_polarization_label * 16 + state_orientation_label
    table = jnp.concatenate(
        [
            labels.astype(F32),
            state_specific_warmth_scaled,
            scattering_lifetimes,
            polarization_propagation_rate,
            jnp.zeros((LOCAL - 6,), F32),
        ]
    ).reshape(1, 4 * LOCAL)
    keep, send = moments(idx, table, excess_phonon_enthalpy)
    received = lax.ppermute(send, "core", [(0, 1), (1, 0)])
    paired = (keep + received.astype(F32)).astype(BF16)
    got = lax.all_to_all(paired, ("space", "zy"), 0, 0, tiled=True)
    own, known, eastward, westward, sums = gathered(
        got, thermal_offset, thermal_conductance_bulk, substance_label
    )
    west = lax.ppermute(eastward, "space", [(i, i + 1) for i in range(7)])
    east = lax.ppermute(westward, "space", [(i + 1, i) for i in range(7)])
    wide, cross, partner = widened(idx, own, known, west, east)
    across = [(2 * p + 1, 2 * p + 2) for p in range(7)]
    cross = lax.ppermute(cross, LINE, across + [(b, a) for a, b in across])
    partner = lax.ppermute(partner, "core", [(0, 1), (1, 0)])
    place = jnp.stack([space, line, core]).astype(jnp.int32)
    temp, flux = solved(place, sums, cross, partner, wide)
    return temp.reshape(16, 8, 64), flux.reshape(3, 16, 8, 64)


def solution(mesh):
    parts = Mesh(mesh.devices.reshape(8, 8, 2), ("space", "zy", "core"))
    modes = P(LINE)
    block = P("space", LINE, None)
    return jax.shard_map(
        per_device,
        mesh=parts,
        in_specs=(P(LINE, "space", None, None), block, modes, modes, modes, modes, P(), block, block),
        out_specs=(block, P(None, "space", LINE, None)),
        check_vma=False,
    )
```

```python
import math

import jax
import jax.numpy as jnp
from jax import lax
from jax.experimental import pallas as pl
from jax.experimental.pallas import tpu as pltpu
from jax.sharding import Mesh, PartitionSpec as P

SWEEPS = 4
STEP = 0.25
MODES = 768
LOCAL = 48
SLAB = 8
NX = 128
NY = 128
NZ = 64
WIN = 5 * LOCAL
DEPTH = 256
EXT = 12
PITCH = 17
PACE = 9
LAYERS = 6 * EXT
DEPTHS = LAYERS // 8
PIECE = DEPTHS * 8
F32 = jnp.float32
BF16 = jnp.bfloat16

SHIFTS = (
    (0, 0), (1, 0), (-1, 0), (2, 0), (-2, 0),
    (0, 1), (1, 1), (-1, 1),
    (0, -1), (1, -1), (-1, -1),
    (0, 2), (0, -2),
)
NS = len(SHIFTS)
BY_Z = tuple(
    (sz, tuple((sy, n) for n, (sy, z) in enumerate(SHIFTS) if z == sz)) for sz in (-2, -1, 0, 1, 2)
)


def lane_iota(shape):
    return lax.broadcasted_iota(jnp.int32, shape, len(shape) - 1)


def mode_rows(table):
    labels = table[0:1, :]
    branch = sum(jnp.where(labels >= 16.0 * b, 1.0, 0.0) for b in range(1, 6))
    orient = labels - 16.0 * branch
    cap = table[1:2, :] / float(MODES)
    rate = 1.0 / table[2:3, :]
    speed = jnp.zeros_like(branch)
    for b in range(6):
        speed = speed + jnp.where(branch == float(b), table[3:4, b : b + 1], 0.0)
    polar = jnp.where(orient >= 4.0, 1.0, 0.0) + jnp.where(orient >= 8.0, 1.0, 0.0)
    polar = polar + jnp.where(orient >= 12.0, 1.0, 0.0)
    turn = orient - 4.0 * polar
    cosine = (2.0 * polar + 1.0) * 0.25 - 1.0
    sine = jnp.sqrt(1.0 - cosine * cosine)
    half = math.sqrt(0.5)
    east = jnp.where((turn == 0.0) | (turn == 3.0), half, -half)
    north = jnp.where(turn < 2.0, half, -half)
    return speed * sine * east, speed * sine * north, speed * cosine, rate, cap


def step_terms(vx, vy, vz, rate):
    cx, cy, cz = (STEP * jnp.abs(v) for v in (vx, vy, vz))
    c0 = 1.0 - cx - cy - cz - STEP * rate
    one = (((0, 0, 0), c0), ((1, 0, 0), cx), ((0, 1, 0), cy), ((0, 0, 1), cz))
    two = (
        ((0, 0, 0), c0 * c0),
        ((1, 0, 0), 2.0 * c0 * cx),
        ((0, 1, 0), 2.0 * c0 * cy),
        ((0, 0, 1), 2.0 * c0 * cz),
        ((2, 0, 0), cx * cx),
        ((0, 2, 0), cy * cy),
        ((0, 0, 2), cz * cz),
        ((1, 1, 0), 2.0 * cx * cy),
        ((1, 0, 1), 2.0 * cx * cz),
        ((0, 1, 1), 2.0 * cy * cz),
    )
    return one, two


def fields_on_rows(vx, vy, vz, rate):
    lanes = rate.shape[1]
    row = lax.broadcasted_iota(jnp.int32, (8, lanes), 0) % 4
    full = [jnp.broadcast_to(v, (8, lanes)) for v in (rate, vx, vy, vz)]
    return jnp.where(
        row == 0, full[0], jnp.where(row == 1, full[1], jnp.where(row == 2, full[2], full[3]))
    )


def build_tables(par_ref, par5, coef):
    par5[...] = jnp.ones(par5.shape, F32)
    for n in range(4):
        for o in range(5):
            par5[n : n + 1, o * LOCAL : (o + 1) * LOCAL] = par_ref[:, n * LOCAL : (n + 1) * LOCAL]
    vx, vy, vz, rate, _ = mode_rows(par5)
    one, two = step_terms(vx, vy, vz, rate)
    weights = fields_on_rows(vx, vy, vz, rate)
    lane = lane_iota((1, DEPTH))
    offset = -2.0 + sum(jnp.where(lane >= o * LOCAL, 1.0, 0.0) for o in range(1, 5))
    inside = lane < WIN
    dx, dy, dz = (jnp.where(v > 0.0, 1.0, -1.0) for v in (vx, vy, vz))
    upper = lax.broadcasted_iota(jnp.int32, (8, DEPTH), 0) < 4

    def total(terms, sy, sz):
        out = jnp.zeros((1, DEPTH), F32)
        for (ax, ay, az), value in terms:
            if ay != abs(sy) or az != abs(sz):
                continue
            hit = inside & (offset == -float(ax) * dx)
            if ay:
                hit = hit & (dy * float(ay) == float(sy))
            if az:
                hit = hit & (dz * float(az) == float(sz))
            out = out + jnp.where(hit, value, 0.0)
        return jnp.broadcast_to(out, (8, DEPTH))

    parts = [
        weights * jnp.where(upper, total(one, sy, sz), total(two, sy, sz)) for sy, sz in SHIFTS
    ]
    rest = parts[0] - parts[0].astype(BF16).astype(F32)
    coef[...] = jnp.concatenate(parts + [rest], axis=0).astype(BF16)


def mode_sums(par5, core):
    vx, vy, vz, rate, cap = mode_rows(par5)
    one, _ = step_terms(vx, vy, vz, rate)
    weights = fields_on_rows(vx, vy, vz, rate)
    gain = STEP * rate * cap
    columns = [weights * gain * one[0][1]]
    for ((ax, ay, az), value), v in zip(one[1:], (vx, vy, vz)):
        for sign in (1.0, -1.0):
            columns.append(weights * gain * jnp.where(v * sign > 0.0, value, 0.0))
    columns.append(weights * gain)
    columns.append(jnp.broadcast_to(cap * rate, weights.shape))
    mine = lane_iota(weights.shape) < LOCAL
    lane = lane_iota((8, 128))
    sums = jnp.zeros((8, 128), F32)
    for n, column in enumerate(columns):
        sums = jnp.where(lane == n, jnp.sum(jnp.where(mine, column, 0.0), axis=1, keepdims=True), sums)
    row = lax.broadcasted_iota(jnp.int32, (8, 128), 0)
    sums = jnp.where((row // 4) == core, sums, 0.0)
    high = sums.astype(BF16).astype(F32)
    return high, pltpu.roll(sums - high, 48, 1)


def moments_kernel(idx_ref, par_ref, e_ref, keep_ref, send_ref, par5, coef, spread, turned, acc, drift):
    z = pl.program_id(0)
    space = idx_ref[0]
    core = idx_ref[1]
    LAYER = NX * PACE

    @pl.when(z == 0)
    def _():
        build_tables(par_ref, par5, coef)
        turned[0 : 2 * LOCAL, :] = jnp.zeros((2 * LOCAL, 128), BF16)
        turned[(NX + 2) * LOCAL :, :] = jnp.zeros((2 * LOCAL + 16, 128), BF16)

        @pl.loop(0, 5 * LAYER // 64)
        def _(r):
            acc[pl.ds(pl.multiple_of(r * 64, 64), 64), :] = jnp.zeros((64, 128), F32)

        acc[13 * LAYER : 14 * LAYER, :] = jnp.zeros((LAYER, 128), F32)

    def turn(c):
        for m in range(LOCAL):
            at = (c * LOCAL + m) * PITCH
            spread[at : at + 16, :] = e_ref[m, 0, 16 * c : 16 * c + 16, :].astype(F32)
        for xx in range(16):
            rows = spread[pl.ds(c * LOCAL * PITCH + xx, LOCAL, stride=PITCH), :].astype(BF16)
            at = (16 * c + xx + 2) * LOCAL
            turned[at : at + LOCAL, :] = rows

    lane = lane_iota((8, 128))

    def moved(value, sy):
        if sy == 0:
            return value
        rolled = pltpu.roll(value, sy % 128, 1)
        return jnp.where(lane >= sy if sy > 0 else lane < 128 + sy, rolled, 0.0)

    def one_pair(x):
            first = turned[x * LOCAL : x * LOCAL + DEPTH, :]
            second = turned[(x + 1) * LOCAL : (x + 1) * LOCAL + DEPTH, :]
            block = jnp.concatenate([first, second], axis=1)
            out = jnp.dot(coef[...], block, preferred_element_type=F32)
            for half in range(2):
                for sz, members in BY_Z:
                    total = None
                    for sy, n in members:
                        part = moved(out[8 * n : 8 * n + 8, 128 * half : 128 * half + 128], sy)
                        if n == 0:
                            part = part + out[8 * NS :, 128 * half : 128 * half + 128]
                        total = part if total is None else total + part
                    at = (z + 3 + sz) * LAYER + (x + half) * PACE
                    if sz == 2:
                        acc[pl.ds(at, 8), :] = total
                    else:
                        acc[pl.ds(at, 8), :] += total

    CHUNKS = NX // 16
    turn(0)
    for c in range(CHUNKS):
        if c + 1 < CHUNKS:
            turn(c + 1)
        for x in range(16 * c, 16 * c + 16, 2):
            one_pair(x)

    @pl.when(z == SLAB - 1)
    def _():
        @pl.when(space == 0)
        def _():
            acc[LAYER : 3 * LAYER, :] = jnp.zeros((2 * LAYER, 128), F32)

        @pl.when(space == 7)
        def _():
            acc[11 * LAYER : 13 * LAYER, :] = jnp.zeros((2 * LAYER, 128), F32)

        row = lax.broadcasted_iota(jnp.int32, (NX, 128), 0)
        col = lane_iota((NX, 128))

        def layer(zo, field, shift=0):
            return acc[pl.ds((zo + 1) * LAYER + field + PACE * shift, NX, stride=PACE), :]

        def divergence(zo):
            east = jnp.where(row < NX - 1, layer(zo, 1, 1), 0.0)
            west = jnp.where(row > 0, layer(zo, 1, -1), 0.0)
            along_y = layer(zo, 2)
            north = jnp.where(col < 127, pltpu.roll(along_y, 127, 1), 0.0)
            south = jnp.where(col > 0, pltpu.roll(along_y, 1, 1), 0.0)
            up = layer(zo + 1, 3)
            down = layer(zo - 1, 3)
            return 0.5 * ((east - west) + (north - south) + (up - down))

        for zo in range(EXT):
            drift[zo * NX : zo * NX + NX, :] = divergence(zo)
        rows = (0, None, 5, 6, 7, 4)
        extras = mode_sums(par5, core)

        def strip(depth, i):
            f, zo = divmod(depth, EXT)
            if rows[f] is None:
                return drift[zo * NX + 16 * i : zo * NX + 16 * i + 16, :]
            return acc[pl.ds((zo + 1) * LAYER + rows[f] + 16 * i * PACE, 16, stride=PACE), :]

        for d in range(DEPTHS):
            for i in range(8):
                tile = jnp.concatenate([strip(8 * d + low, i) for low in range(8)], axis=0).T
                for p in range(8):
                    first, second = tile[16 * p : 16 * p + 8], tile[16 * p + 8 : 16 * p + 16]
                    kept = jnp.where(core == 0, first, second)
                    sent = jnp.where(core == 0, second, first)
                    if d < 2:
                        kept = kept + extras[d]
                        sent = sent + extras[d]
                    keep_ref[8 * i + p, 8 * d : 8 * d + 8, :] = kept
                    send_ref[8 * i + p, 8 * d : 8 * d + 8, :] = sent.astype(BF16)


def moments(idx, table, state):
    whole = pl.BlockSpec((64, PIECE, 128), lambda z: (0, 0, 0))
    return pl.pallas_call(
        moments_kernel,
        grid=(SLAB,),
        in_specs=[
            pl.BlockSpec(memory_space=pltpu.SMEM),
            pl.BlockSpec((1, 4 * LOCAL), lambda z: (0, 0)),
            pl.BlockSpec((LOCAL, 1, NX, NY), lambda z: (0, z, 0, 0)),
        ],
        out_specs=[whole, whole],
        out_shape=[jax.ShapeDtypeStruct((64, PIECE, 128), t) for t in (F32, BF16)],
        scratch_shapes=[
            pltpu.VMEM((8, DEPTH), F32),
            pltpu.VMEM((NS * 8 + 8, DEPTH), BF16),
            pltpu.VMEM((8 * LOCAL * PITCH + 8, 128), F32),
            pltpu.VMEM(((NX + 4) * LOCAL + 16, 128), BF16),
            pltpu.VMEM((14 * NX * PACE, 128), F32),
            pltpu.VMEM((EXT * NX, 128), F32),
        ],
        compiler_params=pltpu.CompilerParams(vmem_limit_bytes=48 << 20),
        cost_estimate=pl.CostEstimate(flops=20_000_000_000, bytes_accessed=16_000_000, transcendentals=0),
        name="moments",
    )(idx, table, state)


def gather_kernel(
    got_ref, temp_ref, bulk_ref, label_ref, own_ref, known_ref, east_ref, west_ref, sums_ref, total
):
    lane = lane_iota((8, 128))
    group = lane // 32
    eighth = (lane % 32) // 8
    for s in range(8):
        for d in range(DEPTHS):
            value = got_ref[8 * s, 8 * d : 8 * d + 8, :].astype(F32)
            for q in range(1, 8):
                value = value + got_ref[8 * s + q, 8 * d : 8 * d + 8, :].astype(F32)
            total[s * DEPTHS + d] = value

    sums = total[0] + pltpu.roll(total[1], 80, 1)
    sums_ref[...] = sums + pltpu.roll(sums, 4, 0)

    def layer(s, f, zo, quarter):
        depth = f * EXT + zo
        turn = (32 * quarter + 8 - 16 * (depth % 8)) % 128
        value = total[s * DEPTHS + depth // 8]
        return pltpu.roll(value, turn, 1) if turn else value

    for f in range(6):
        reach = 1 if f == 0 else 2
        for zz in range(16):
            value = None
            for quarter in range(4):
                z = quarter * 16 + zz
                s = z // 8
                part = layer(s, f, z % 8 + 2, quarter)
                if z % 8 < reach and s > 0:
                    part = part + layer(s - 1, f, z % 8 + 10, quarter)
                if z % 8 > 7 - reach and s < 7:
                    part = part + layer(s + 1, f, z % 8 - 6, quarter)
                value = part if quarter == 0 else jnp.where(group >= quarter, part, value)
            own_ref[f, zz] = value

    wide_group = lane_iota((16, 128)) // 32

    def block_of(n, read):
        cells = jnp.concatenate([read(pl.ds(y, 16, stride=8)) for y in range(8)], axis=0).T
        for y in range(8):
            value = None
            for quarter in range(4):
                turn = (32 * quarter + 8 - 16 * y) % 128
                part = cells[16 * quarter : 16 * quarter + 16]
                part = pltpu.roll(part, turn, 1) if turn else part
                value = part if quarter == 0 else jnp.where(wide_group >= quarter, part, value)
            known_ref[n, pl.ds(y, 16, stride=8), :] = value

    block_of(0, lambda rows: temp_ref[rows, :])
    block_of(1, lambda rows: bulk_ref[rows, :] * jnp.where(label_ref[rows, :] == 1, 0.1, 1.0))

    for n in range(7):

        def cells(zz):
            if n < 5:
                return own_ref[n, zz]
            return known_ref[n - 5, 8 * zz : 8 * zz + 8, :]

        for h in range(4):
            rows = slice((n * 4 + h) * 8, (n * 4 + h) * 8 + 8)
            for ref, first in ((east_ref, 16), (west_ref, 8)):
                packed = None
                for k in range(4):
                    turn = (8 * k - first) % 128
                    value = cells(4 * h + k)
                    value = pltpu.roll(value, turn, 1) if turn else value
                    packed = value if k == 0 else jnp.where(eighth == k, value, packed)
                ref[rows, :] = packed.astype(BF16)


def gathered(got, temp, bulk, label):
    flat = [value.reshape(128, NZ) for value in (temp, bulk, label)]
    return pl.pallas_call(
        gather_kernel,
        out_shape=[
            jax.ShapeDtypeStruct((6, 16, 8, 128), F32),
            jax.ShapeDtypeStruct((2, 128, 128), F32),
            jax.ShapeDtypeStruct((7 * 32, 128), BF16),
            jax.ShapeDtypeStruct((7 * 32, 128), BF16),
            jax.ShapeDtypeStruct((8, 128), F32),
        ],
        scratch_shapes=[pltpu.VMEM((8 * DEPTHS, 8, 128), F32)],
        compiler_params=pltpu.CompilerParams(vmem_limit_bytes=16 << 20),
        name="gather",
    )(got, *flat)


FULL = (1, 5, 6)
HALVES = ((0, 2), (3, 4))
HALO = (len(FULL) + len(HALVES)) * 128


def widen_kernel(idx_ref, own_ref, known_ref, west_ref, east_ref, wide_ref, cross_ref, partner_ref):
    part = lane_iota((8, 128)) % 32
    row = lax.broadcasted_iota(jnp.int32, (8, 128), 0)
    core = idx_ref[1]

    def cells(n, zz):
        at = (n * 4 + zz // 4) * 8
        k = zz % 4
        west = west_ref[at : at + 8, :].astype(F32)
        west = pltpu.roll(west, 128 - 8 * k, 1) if k else west
        east = east_ref[at : at + 8, :].astype(F32)
        east = pltpu.roll(east, 24 - 8 * k, 1) if k < 3 else east
        own = own_ref[n, zz] if n < 5 else known_ref[n - 5, 8 * zz : 8 * zz + 8, :]
        value = jnp.where(part < 8, west, jnp.where(part < 24, own, east))
        wide_ref[n, zz] = value
        return value

    for zz in range(16):
        wide_ref[7, zz] = own_ref[5, zz]
        for u, n in enumerate(FULL):
            value = cells(n, zz).astype(BF16)
            at = (u * 16 + zz) * 8
            cross_ref[at : at + 8, :] = value
            partner_ref[at : at + 8, :] = value
        for u, (n, m) in enumerate(HALVES):
            value = cells(n, zz)
            other = pltpu.roll(cells(m, zz), 4, 0)
            southward = jnp.where(row < 4, value, other)
            northward = jnp.where(row < 4, other, value)
            at = ((len(FULL) + u) * 16 + zz) * 8
            cross_ref[at : at + 8, :] = jnp.where(core == 0, southward, northward).astype(BF16)
            partner_ref[at : at + 8, :] = jnp.where(core == 0, northward, southward).astype(BF16)


def widened(idx, own, known, west, east):
    vmem = pl.BlockSpec(memory_space=pltpu.VMEM)
    return pl.pallas_call(
        widen_kernel,
        in_specs=[pl.BlockSpec(memory_space=pltpu.SMEM)] + [vmem] * 4,
        out_shape=[
            jax.ShapeDtypeStruct((8, 16, 8, 128), F32),
            jax.ShapeDtypeStruct((HALO, 128), BF16),
            jax.ShapeDtypeStruct((HALO, 128), BF16),
        ],
        compiler_params=pltpu.CompilerParams(vmem_limit_bytes=8 << 20),
        name="widen",
    )(idx, own, known, west, east)


def solve_kernel(idx_ref, sums_vmem, cross_ref, partner_ref, wide_ref, temp_ref, flux_ref, lines, sums_ref, sem):
    copy = pltpu.make_async_copy(sums_vmem, sums_ref, sem)
    copy.start()
    shape = (16, 24, 128)
    lane = lane_iota((1, 24, 128))
    x = lane % 32 + (idx_ref[0] * 16 - 8)
    y = lax.broadcasted_iota(jnp.int32, (1, 24, 128), 1) + (idx_ref[1] * 8 - 8)
    inside = jnp.where((x >= 0) & (x < NX) & (y >= 0) & (y < NY), 1.0, 0.0)
    group = lane_iota((1, 24, 128)) // 32

    def sent(ref, f):
        if f in FULL:
            u = FULL.index(f)
            return ref[u * 128 : u * 128 + 128, :].astype(F32).reshape(16, 8, 128)
        u, second = next((u, pair.index(f)) for u, pair in enumerate(HALVES) if f in pair)
        at = (len(FULL) + u) * 128
        value = ref[at : at + 128, :].astype(F32).reshape(16, 8, 128)
        return pltpu.roll(value, 4, 1) if second else value

    def field(f):
        cross = sent(cross_ref, f)
        partner = sent(partner_ref, f)
        first = idx_ref[2] == 0
        south = jnp.where(first, cross, partner)
        north = jnp.where(first, partner, cross)
        return jnp.concatenate([south, wide_ref[f], north], axis=1)

    def known(n):
        return field(5 + n)

    def east(v):
        return pltpu.roll(v, 127, 2)

    def west(v):
        return pltpu.roll(v, 1, 2)

    def north(v):
        return jnp.concatenate([v[:, 1:], jnp.zeros((16, 1, 128), F32)], axis=1)

    def south(v):
        return jnp.concatenate([jnp.zeros((16, 1, 128), F32), v[:, :-1]], axis=1)

    def above(v):
        edge = jnp.where(group < 3, pltpu.roll(v[0:1], 96, 2), 0.0)
        return jnp.concatenate([v[1:], edge], axis=0)

    def below(v):
        edge = jnp.where(group > 0, pltpu.roll(v[15:16], 32, 2), 0.0)
        return jnp.concatenate([edge, v[:-1]], axis=0)

    kappa = known(1)

    def face(a, b):
        summed = a + b
        positive = summed > 0.0
        return jnp.where(positive, 2.0 * a * b / jnp.where(positive, summed, 1.0), 0.0)

    face_e = face(kappa, east(kappa))
    face_n = face(kappa, north(kappa))
    face_u = face(kappa, above(kappa))
    face_w = west(face_e)
    face_s = south(face_n)
    face_d = below(face_u)

    copy.wait()
    total = jnp.full((1, 24, 128), sums_ref[0, 8], F32)
    theta = total + 6.0
    sigma = theta / 6.0

    def operator(v):
        out = face_e * (east(v) - v) + face_w * (west(v) - v)
        out = out + face_n * (north(v) - v) + face_s * (south(v) - v)
        out = out + face_u * (above(v) - v) + face_d * (below(v) - v)
        return total * v - out

    def chebyshev(rhs):
        rho = 1.0 / sigma
        residual = rhs
        direction = rhs / theta
        correction = direction
        for sweep in range(SWEEPS - 1):
            residual = residual - operator(direction)
            rho_next = 1.0 / (2.0 * sigma - rho)
            direction = rho_next * rho * direction + 2.0 * rho_next / 6.0 * residual
            rho = rho_next
            correction = correction + direction
        return correction

    temp = known(0)
    moved = (temp, west(temp), east(temp), south(temp), north(temp), below(temp), above(temp))
    gain = [sums_ref[k, 7] for k in range(4)]
    rhs = 0.5 * (
        gain[1] * (moved[2] - moved[1]) + gain[2] * (moved[4] - moved[3]) + gain[3] * (moved[6] - moved[5])
    )
    rhs = -(field(1) + rhs)
    once = (field(0) + gain[0] * temp) / total + chebyshev(rhs)

    def second(k, part):
        value = part + gain[k] * once
        for s in range(7):
            value = value + sums_ref[k, s] * moved[s]
        return value

    flux = [second(k, field(k + 1)) * inside for k in (1, 2, 3)]
    own = wide_ref[7]
    energy = second(0, jnp.concatenate([own, own, own], axis=1))
    rhs = -0.5 * (
        (east(flux[0]) - west(flux[0])) + (north(flux[1]) - south(flux[1])) + (above(flux[2]) - below(flux[2]))
    )
    twice = energy / total + chebyshev(rhs)
    quarter = lane_iota((16, 128)) // 16

    def write(n, value, store):
        for zz in range(16):
            lines[n, zz * PACE : zz * PACE + 8, :] = value[zz, 8:16]
        rows = [lines[n, pl.ds(y, 16, stride=PACE), :] for y in range(8)]
        turned = jnp.concatenate(rows, axis=0).T
        for y in range(8):
            out = None
            for q in range(4):
                part = turned[32 * q + 8 : 32 * q + 24]
                move = (16 * (q - y)) % 128
                part = pltpu.roll(part, move, 1) if move else part
                out = part if q == 0 else jnp.where(quarter >= q, part, out)
            store(y, out[:, :64])

    def store_temp(y, out):
        temp_ref[pl.ds(y, 16, stride=8), :] = out

    write(0, twice, store_temp)
    for n in range(3):

        def store_flux(y, out, n=n):
            flux_ref[n, pl.ds(y, 16, stride=8), :] = out

        write(n + 1, flux[n], store_flux)


def solved(idx, sums, cross, partner, wide):
    vmem = pl.BlockSpec(memory_space=pltpu.VMEM)
    return pl.pallas_call(
        solve_kernel,
        in_specs=[pl.BlockSpec(memory_space=pltpu.SMEM)] + [vmem] * 4,
        out_specs=[vmem, vmem],
        out_shape=[
            jax.ShapeDtypeStruct((128, 64), F32),
            jax.ShapeDtypeStruct((3, 128, 64), F32),
        ],
        scratch_shapes=[
            pltpu.VMEM((4, 16 * PACE, 128), F32),
            pltpu.SMEM((8, 128), F32),
            pltpu.SemaphoreType.DMA(()),
        ],
        compiler_params=pltpu.CompilerParams(vmem_limit_bytes=16 << 20),
        name="solve",
    )(idx, sums, cross, partner, wide)


LINE = ("zy", "core")


def per_device(
    excess_phonon_enthalpy,
    thermal_offset,
    state_specific_warmth_scaled,
    scattering_lifetimes,
    state_polarization_label,
    state_orientation_label,
    polarization_propagation_rate,
    thermal_conductance_bulk,
    substance_label,
):
    space = lax.axis_index("space")
    core = lax.axis_index("core")
    line = lax.axis_index("zy") * 2 + core
    idx = jnp.stack([space, core]).astype(jnp.int32)
    labels = state_polarization_label * 16 + state_orientation_label
    table = jnp.concatenate(
        [
            labels.astype(F32),
            state_specific_warmth_scaled,
            scattering_lifetimes,
            polarization_propagation_rate,
            jnp.zeros((LOCAL - 6,), F32),
        ]
    ).reshape(1, 4 * LOCAL)
    keep, send = moments(idx, table, excess_phonon_enthalpy)
    received = lax.ppermute(send, "core", [(0, 1), (1, 0)])
    paired = (keep + received.astype(F32)).astype(BF16)
    got = lax.all_to_all(paired, ("space", "zy"), 0, 0, tiled=True)
    own, known, eastward, westward, sums = gathered(
        got, thermal_offset, thermal_conductance_bulk, substance_label
    )
    west = lax.ppermute(eastward, "space", [(i, i + 1) for i in range(7)])
    east = lax.ppermute(westward, "space", [(i + 1, i) for i in range(7)])
    wide, cross, partner = widened(idx, own, known, west, east)
    across = [(2 * p + 1, 2 * p + 2) for p in range(7)]
    cross = lax.ppermute(cross, LINE, across + [(b, a) for a, b in across])
    partner = lax.ppermute(partner, "core", [(0, 1), (1, 0)])
    place = jnp.stack([space, line, core]).astype(jnp.int32)
    temp, flux = solved(place, sums, cross, partner, wide)
    return temp.reshape(16, 8, 64), flux.reshape(3, 16, 8, 64)


def solution(mesh):
    parts = Mesh(mesh.devices.reshape(8, 8, 2), ("space", "zy", "core"))
    modes = P(LINE)
    block = P("space", LINE, None)
    return jax.shard_map(
        per_device,
        mesh=parts,
        in_specs=(P(LINE, "space", None, None), block, modes, modes, modes, modes, P(), block, block),
        out_specs=(block, P(None, "space", LINE, None)),
        check_vma=False,
    )
```
